64 devices in a mesh: dp: 4 (over x, y), sp: 16 (over z, core).
Axes of the slice: x: 2, y: 2, z: 8, core: 2. Of those that a mesh axis runs over, the one named last changes fastest.
The devices are a block of a 4x4x8 slice.
Arguments:
- x: bfloat16 [8192, 4096], P(('dp', 'sp')), parts along dimension 0
- gain: bfloat16 [4096], replicated
- wq: bfloat16 [4096, 6144], replicated
- wk: bfloat16 [4096, 1024], replicated
- wv: bfloat16 [4096, 1024], replicated
- wo: bfloat16 [6144, 4096], replicated
Outputs:
- output: bfloat16 [8192, 4096], P(('dp', 'sp')), parts along dimension 0
There are 4 independent parts. The reference program is written for one: setup_inputs(seed, part) draws one part's arguments, and reference() takes and returns one part's arrays. A program takes and returns all parts, laid end to end along the dimension named above; an argument that names none is the same for every part.
All inputs are finite; a program needn't handle non-finite values.
Results may differ from the reference program's by a relative error of at most 0.012.
Values are sent between devices in bfloat16 or wider.
A program may use at most 768 MiB of HBM per device.

```python
import jax
import jax.numpy as jnp
from jax import lax

ROWS = 2048
D = 4096
HEADS = 48
KV_HEADS = 8
HEAD = 128
THETA = 10000


def setup_inputs(seed: int = 0, part: int = 0) -> dict:
    kx, kn, kq, kk, kv, ko = jax.random.split(jax.random.key(seed), 6)

    def weights(key, rows, columns):
        return jax.random.normal(key, (rows, columns), jnp.float32) * rows**-0.5

    drawn = {
        "x": jax.random.normal(jax.random.fold_in(kx, part), (ROWS, D), jnp.float32),
        "gain": 1 + 0.1 * jax.random.normal(kn, (D,), jnp.float32),
        "wq": 2 * weights(kq, D, HEADS * HEAD),
        "wk": 2 * weights(kk, D, KV_HEADS * HEAD),
        "wv": 4 * weights(kv, D, KV_HEADS * HEAD),
        "wo": weights(ko, HEADS * HEAD, D),
    }
    return {k: v.astype(jnp.bfloat16) for k, v in drawn.items()}


def normed(x, gain):
    wide = x.astype(jnp.float32)
    scale = lax.rsqrt(jnp.mean(wide * wide, -1, keepdims=True) + 1e-6)
    return (wide * scale * gain.astype(jnp.float32)).astype(jnp.bfloat16)


def turned(t, place, theta):
    half = t.shape[-1] // 2
    angle = place.astype(jnp.float32)[:, None] * theta ** (-jnp.arange(half, dtype=jnp.float32) / half)
    cos, sin = jnp.cos(angle)[:, None], jnp.sin(angle)[:, None]
    a, b = t[..., :half].astype(jnp.float32), t[..., half:].astype(jnp.float32)
    return jnp.concatenate([a * cos - b * sin, b * cos + a * sin], -1).astype(jnp.bfloat16)


def matmul(a, w):
    return jnp.dot(a, w, preferred_element_type=jnp.float32).astype(jnp.bfloat16)


def einsum(form, a, b):
    return jnp.einsum(form, a.astype(jnp.float32), b.astype(jnp.float32))


def attention(q, k, v):
    scores = einsum("tgsd,ugd->gstu", q, k) * q.shape[-1] ** -0.5
    token = jnp.arange(q.shape[0])
    scores = jnp.where(token[:, None] >= token, scores, -jnp.inf)
    weights = jax.nn.softmax(scores, -1).astype(jnp.bfloat16)
    return einsum("gstu,ugd->tgsd", weights, v).astype(jnp.bfloat16)


def reference(x, gain, wq, wk, wv, wo):
    a, place = normed(x, gain), jnp.arange(ROWS)
    q = turned(matmul(a, wq).reshape(ROWS, HEADS, HEAD), place, THETA).reshape(ROWS, KV_HEADS, -1, HEAD)
    k = turned(matmul(a, wk).reshape(ROWS, KV_HEADS, HEAD), place, THETA)
    v = matmul(a, wv).reshape(ROWS, KV_HEADS, HEAD)
    seen = attention(q, k, v).reshape(ROWS, HEADS * HEAD)
    return (x.astype(jnp.float32) + jnp.dot(seen, wo, preferred_element_type=jnp.float32)).astype(jnp.bfloat16)
```

```python
import functools

import jax
import jax.numpy as jnp
import numpy as np
from jax import lax
from jax.experimental import pallas as pl
from jax.experimental.pallas import tpu as pltpu
from jax.sharding import PartitionSpec as P

HEAD = 128
THETA = 10000
LOG2E = 1.4426950408889634
WIDE = 256
SLOTS = 6
STRIP = 512
OUT = 512
MESH = pl.DeviceIdType.MESH


def _dot(a, b, ca=1, cb=0):
    return lax.dot_general(a, b, (((ca,), (cb,)), ((), ())), preferred_element_type=jnp.float32)


def _kernel(nz, x_ref, gain_ref, freq_ref, wq_ref, wk_ref, wv_ref, wo_ref, y_ref, x_s, a_s, pool, wo_s, kv_s, q_s, top_s, mix_s, acc_s, own_s,
            oth_s, y_s, cos_s, sin_s, w_sem, wo_sem, x_sem, ring_send, ring_recv, seen_send, seen_recv, y_sem):
    me = lax.axis_index("sp")
    core, z = lax.rem(me, 2), lax.div(me, 2)
    mate = me + 1 - 2 * core
    right, left = 2 * lax.rem(z + 1, nz) + core, 2 * lax.rem(z + nz - 1, nz) + core
    own, d = x_ref.shape
    both = 2 * own
    groups = kv_s.shape[1]
    g = q_s.shape[0] // groups
    per = groups // 2
    rows = own_s.shape[2]
    half = y_s.shape[2]
    far = nz // 2
    tiles = q_s.shape[0] * HEAD // WIDE
    e = HEAD**-0.5 * LOG2E

    def load(ref, column, slot):
        return pltpu.make_async_copy(ref.at[:, pl.ds(pl.multiple_of(column, WIDE), WIDE)], pool.at[slot], w_sem.at[slot])

    def wq_tile(i):
        return load(wq_ref, core * (q_s.shape[0] * HEAD) + i * WIDE, lax.rem(i + 2 * groups // 2, SLOTS))

    def wk_tile(p):
        return load(wk_ref, core * (groups * HEAD) + p * WIDE, 2 * p)

    def wv_tile(p):
        return load(wv_ref, core * (groups * HEAD) + p * WIDE, 2 * p + 1)

    def wo_tile(s, o):
        who = core if o == 0 else 1 - core
        row = pl.multiple_of(who * (2 * rows) + s * rows, 128)
        return pltpu.make_async_copy(wo_ref.at[pl.ds(row, rows), pl.ds(pl.multiple_of(core * half, 128), half)], wo_s.at[s, o], wo_sem.at[s, o])

    def to(src, dst, send, recv, device):
        return pltpu.make_async_remote_copy(src_ref=src, dst_ref=dst, send_sem=send, recv_sem=recv, device_id={"sp": device}, device_id_type=MESH)

    def hop(k, h, way):
        src, dst = (k - 1, k) if way == 0 else (lax.rem(nz + 1 - k, nz), nz - k)
        return to(kv_s.at[src, h], kv_s.at[dst, h], ring_send.at[way, k, h], ring_recv.at[way, k, h], right if way == 0 else left)

    def last_hop(h, way):
        src = far - 1 if way == 0 else nz + 1 - far
        return to(kv_s.at[src, h, way], kv_s.at[far, h, way], ring_send.at[way, far, h], ring_recv.at[way, far, h], right if way == 0 else left)

    x_own = pltpu.make_async_copy(x_ref, x_s.at[core], x_sem.at[0])
    x_mate = to(x_ref, x_s.at[core], x_sem.at[1], x_sem.at[2], mate)

    x_own.start()
    for p in range(2):
        wk_tile(p).start()
        wv_tile(p).start()
    for i in range(SLOTS - 4):
        wq_tile(i).start()

    barrier = pltpu.get_barrier_semaphore()
    for device in (mate, left, right):
        pl.semaphore_signal(barrier, inc=1, device_id={"sp": device}, device_id_type=MESH)
    pl.semaphore_wait(barrier, 3)
    x_mate.start()

    place = lax.broadcasted_iota(jnp.int32, (both, HEAD), 0) + z * both
    angle = place.astype(jnp.float32) * freq_ref[...]
    sign = jnp.where(lax.broadcasted_iota(jnp.int32, (both, HEAD), 1) < HEAD // 2, -1.0, 1.0)
    cos_s[...] = jnp.cos(angle)
    sin_s[...] = jnp.sin(angle) * sign

    def norm(who):
        def chunk(r, _):
            wide = x_s[who, pl.ds(pl.multiple_of(r * 16, 16), 16), :].astype(jnp.float32)
            scale = lax.rsqrt(jnp.mean(wide * wide, -1, keepdims=True) + 1e-6)
            a = (wide * scale * gain_ref[...].astype(jnp.float32)).astype(jnp.bfloat16)
            a_s[pl.ds(pl.multiple_of(who * own + r * 16, 16), 16), :] = a

        lax.fori_loop(0, own // 16, chunk, None)

    x_own.wait()
    norm(core)
    x_mate.wait_recv()
    norm(1 - core)

    def turn(t):
        t = t.astype(jnp.bfloat16).astype(jnp.float32)
        return (t * cos_s[...] + pltpu.roll(t, HEAD // 2, 1) * sin_s[...]).astype(jnp.bfloat16)

    def start_own(s):
        for h in range(s * per, (s + 1) * per):
            hop(1, h, 0).start()
            hop(1, h, 1).start()

    for p in range(2):
        wk_tile(p).wait()
        got = _dot(a_s[...], pool[2 * p])
        for i in range(2):
            kv_s[0, 2 * p + i, 0] = turn(got[:, i * HEAD : (i + 1) * HEAD])
        wv_tile(p).wait()
        got = _dot(a_s[...], pool[2 * p + 1]).astype(jnp.bfloat16)
        for i in range(2):
            kv_s[0, 2 * p + i, 1] = got[:, i * HEAD : (i + 1) * HEAD]
        if p == 0:
            start_own(0)
        wq_tile(SLOTS - 4 + 2 * p).start()
        wq_tile(SLOTS - 3 + 2 * p).start()

    def queries(i, more):
        wq_tile(i).wait()
        got = _dot(a_s[...], pool[lax.rem(i + groups, SLOTS)])
        for n in range(2):
            q_s[2 * i + n] = turn(got[:, n * HEAD : (n + 1) * HEAD])
        if more:
            wq_tile(i + SLOTS).start()

    lax.fori_loop(0, tiles // 2, lambda i, _: queries(i, True), None)
    for s in range(2):
        for o in range(2):
            wo_tile(s, o).start()

    def attend(j, h, slots, diagonal=False):
        keys = [kv_s[n, h, 0] for n in slots]
        values = jnp.concatenate([kv_s[n, h, 1].T for n in slots], axis=1)
        values = jnp.concatenate([values, jnp.ones((8, values.shape[1]), values.dtype)], axis=0)
        n = STRIP // both
        strips = range(0, g * both, STRIP)
        scores = []
        for at in strips:
            q = q_s[pl.ds(g * h + at // both, n)].reshape(STRIP, HEAD)
            scores.append([_dot(k, q, 1, 1) for k in keys])
        weights, keeps = [], []
        for at, parts in zip(strips, scores):
            if diagonal:
                seen = lax.rem(lax.broadcasted_iota(jnp.int32, (both, STRIP), 1), both) >= lax.broadcasted_iota(jnp.int32, (both, STRIP), 0)
                parts = [jnp.where(seen, parts[0], -jnp.inf)]
            old = None if diagonal else top_s[j, :, at : at + STRIP]
            top = functools.reduce(jnp.maximum, [s.max(axis=0, keepdims=True) for s in parts] + ([] if diagonal else [old]))
            top_s[j, :, at : at + STRIP] = top
            weights.append(jnp.concatenate([jnp.exp2((s - top) * e).astype(jnp.bfloat16) for s in parts], axis=0))
            keeps.append(None if diagonal else jnp.exp2((old - top) * e))
        for at, w, keep in zip(strips, weights, keeps):
            got = _dot(values, w)
            mix_s[j, :, at : at + STRIP] = got if diagonal else mix_s[j, :, at : at + STRIP] * keep + got

    def finish(s):
        for j in range(per):
            for n in range(g):
                at = slice(n * both, (n + 1) * both)
                out = mix_s[j, :HEAD, at] * (1 / mix_s[j, HEAD : HEAD + 1, at])
                column = (j * g + n) * HEAD
                own_s[s, :, column : column + HEAD] = out.T.astype(jnp.bfloat16)
        seen(s).start()

    def seen(s):
        return to(own_s.at[s], oth_s.at[s], seen_send.at[s], seen_recv.at[s], mate)

    def stage(s, beside):
        base = s * per
        for j in range(per):
            attend(j, base + j, [0], diagonal=True)

        def arrive(n, _):
            k, j = 1 + lax.div(n, per), lax.rem(n, per)
            h = base + j
            for way in range(2):
                hop(k, h, way).wait_recv()

            @pl.when(k < far - 1)
            def _():
                for way in range(2):
                    hop(k + 1, h, way).start()

            @pl.when(k == far - 1)
            def _():
                for way in range(2):
                    last_hop(h, way).start()

            beside(n)

            @pl.when(z + k >= nz)
            def _():
                attend(j, h, [k, nz - k])

            @pl.when((z + k < nz) & (z >= k))
            def _():
                attend(j, h, [k])

        lax.fori_loop(0, (far - 1) * per, arrive, None)
        if s == 0:
            start_own(1)

        def end(j, _):
            for way in range(2):
                last_hop(base + j, way).wait_recv()

            @pl.when(z >= far)
            def _():
                attend(j, base + j, [far])

        lax.fori_loop(0, per, end, None)
        finish(s)

    def column_tile(ct):
        return pl.ds(pl.multiple_of(ct * OUT, OUT), OUT)

    def project(s, o, at):
        return _dot((own_s, oth_s)[o][s], wo_s[s, o, :, at])

    stage(0, lambda n: queries(tiles // 2 + n, False))

    for o in range(2):
        wo_tile(0, o).wait()

    def first_half(n):
        @pl.when(n == 0)
        def _():
            seen(0).wait_recv()

        @pl.when(n < half // OUT)
        def _():
            at = column_tile(n)
            acc_s[:, at] = project(0, 0, at) + project(0, 1, at)

    stage(1, first_half)

    for o in range(2):
        wo_tile(1, o).wait()

    def mine(ct, _):
        at = column_tile(ct)
        acc_s[:, at] += project(1, 0, at)

    lax.fori_loop(0, half // OUT, mine, None)
    seen(1).wait_recv()

    def theirs(ct, _):
        at = column_tile(ct)
        total = acc_s[:, at] + project(1, 1, at)
        for i in range(2):
            x = x_s[i, :, pl.ds(pl.multiple_of(core * half + ct * OUT, OUT), OUT)].astype(jnp.float32)
            y_s[i, :, at] = (x + total[i * own : (i + 1) * own]).astype(jnp.bfloat16)

    lax.fori_loop(0, half // OUT, theirs, None)
    columns = y_ref.at[:, pl.ds(pl.multiple_of(core * half, 128), half)]
    y_mate = to(y_s.at[1 - core], columns, y_sem.at[0], y_sem.at[1], mate)
    y_own = pltpu.make_async_copy(y_s.at[core], columns, y_sem.at[2])
    y_mate.start()
    y_own.start()

    x_mate.wait_send()
    for s in range(2):
        seen(s).wait_send()

    def sent(h, _):
        for way in range(2):
            for k in range(1, far):
                hop(k, h, way).wait_send()
            last_hop(h, way).wait_send()

    lax.fori_loop(0, groups, sent, None)
    y_own.wait()
    y_mate.wait()


def solution(mesh):
    nz = mesh.shape["sp"] // 2

    def step(x, gain, wq, wk, wv, wo):
        own, d = x.shape
        both = 2 * own
        heads, groups = wq.shape[1] // HEAD // 2, wk.shape[1] // HEAD // 2
        g, per, half = heads // groups, groups // 2, d // 2
        rows = heads * HEAD // 2
        far = nz // 2
        freq = np.float32(THETA) ** (-(np.arange(HEAD) % (HEAD // 2)).astype(np.float32) / (HEAD // 2))
        vmem, hbm = pl.BlockSpec(memory_space=pltpu.VMEM), pl.BlockSpec(memory_space=pl.ANY)
        low = jnp.bfloat16
        dma = pltpu.SemaphoreType.DMA
        return pl.pallas_call(
            functools.partial(_kernel, nz),
            out_shape=jax.ShapeDtypeStruct((own, d), low),
            in_specs=[hbm, vmem, vmem, hbm, hbm, hbm, hbm],
            out_specs=hbm,
            scratch_shapes=[
                pltpu.VMEM((2, own, d), low),
                pltpu.VMEM((both, d), low),
                pltpu.VMEM((SLOTS, d, WIDE), low),
                pltpu.VMEM((2, 2, rows, half), low),
                pltpu.VMEM((nz, groups, 2, both, HEAD), low),
                pltpu.VMEM((heads, both, HEAD), low),
                pltpu.VMEM((per, 1, g * both), jnp.float32),
                pltpu.VMEM((per, HEAD + 8, g * both), jnp.float32),
                pltpu.VMEM((both, half), jnp.float32),
                pltpu.VMEM((2, both, rows), low),
                pltpu.VMEM((2, both, rows), low),
                pltpu.VMEM((2, own, half), low),
                pltpu.VMEM((both, HEAD), jnp.float32),
                pltpu.VMEM((both, HEAD), jnp.float32),
                dma((SLOTS,)),
                dma((2, 2)),
                dma((3,)),
                dma((2, far + 1, groups)),
                dma((2, far + 1, groups)),
                dma((2,)),
                dma((2,)),
                dma((3,)),
            ],
            compiler_params=pltpu.CompilerParams(collective_id=0, has_side_effects=True, vmem_limit_bytes=67043328),
        )(x, gain.reshape(1, d), jnp.asarray(freq, jnp.float32)[None], wq, wk, wv, wo)

    tokens, whole = P(("dp", "sp"), None), P(None, None)
    return jax.shard_map(
        step,
        mesh=mesh,
        in_specs=(tokens, P(None), whole, whole, whole, whole),
        out_specs=tokens,
        check_vma=False,
    )
```

```python
import functools

import jax
import jax.numpy as jnp
import numpy as np
from jax import lax
from jax.experimental import pallas as pl
from jax.experimental.pallas import tpu as pltpu
from jax.sharding import PartitionSpec as P

HEAD = 128
THETA = 10000
LOG2E = 1.4426950408889634
WIDE = 256
SLOTS = 6
STRIP = 512
OUT = 512
MESH = pl.DeviceIdType.MESH


def _dot(a, b, ca=1, cb=0):
    return lax.dot_general(a, b, (((ca,), (cb,)), ((), ())), preferred_element_type=jnp.float32)


def _kernel(nz, x_ref, gain_ref, freq_ref, wq_ref, wk_ref, wv_ref, wo_ref, y_ref, x_s, a_s, pool, wo_s, kv_s, q_s, top_s, mix_s, acc_s, own_s,
            oth_s, y_s, cos_s, sin_s, w_sem, wo_sem, x_sem, ring_send, ring_recv, half_send, half_recv, seen_send, seen_recv, y_sem, own_sem):
    me = lax.axis_index("sp")
    core, z = lax.rem(me, 2), lax.div(me, 2)
    mate = me + 1 - 2 * core
    right, left = 2 * lax.rem(z + 1, nz) + core, 2 * lax.rem(z + nz - 1, nz) + core
    own, d = x_ref.shape
    both = 2 * own
    groups = kv_s.shape[1]
    g = q_s.shape[0] // groups
    per = groups // 2
    rows = own_s.shape[2]
    half = y_s.shape[2]
    far = nz // 2
    tiles = q_s.shape[0] * HEAD // WIDE
    e = HEAD**-0.5 * LOG2E

    def load(ref, column, slot):
        return pltpu.make_async_copy(ref.at[:, pl.ds(pl.multiple_of(column, WIDE), WIDE)], pool.at[slot], w_sem.at[slot])

    def wq_tile(i):
        return load(wq_ref, core * (q_s.shape[0] * HEAD) + i * WIDE, lax.rem(i + 2 * groups // 2, SLOTS))

    def wk_tile(p):
        return load(wk_ref, core * (groups * HEAD) + p * WIDE, 2 * p)

    def wv_tile(p):
        return load(wv_ref, core * (groups * HEAD) + p * WIDE, 2 * p + 1)

    def wo_tile(s, o):
        who = core if o == 0 else 1 - core
        row = pl.multiple_of(who * (2 * rows) + s * rows, 128)
        return pltpu.make_async_copy(wo_ref.at[pl.ds(row, rows), pl.ds(pl.multiple_of(core * half, 128), half)], wo_s.at[s, o], wo_sem.at[s, o])

    def to(src, dst, send, recv, device):
        return pltpu.make_async_remote_copy(src_ref=src, dst_ref=dst, send_sem=send, recv_sem=recv, device_id={"sp": device}, device_id_type=MESH)

    def hop(k, h, way):
        src, dst = (k - 1, k) if way == 0 else (lax.rem(nz + 1 - k, nz), nz - k)
        return to(kv_s.at[src, h], kv_s.at[dst, h], ring_send.at[way, k, h], ring_recv.at[way, k, h], right if way == 0 else left)

    def last_hop(h, way):
        src = far - 1 if way == 0 else nz + 1 - far
        return to(kv_s.at[src, h, way], kv_s.at[far, h, way], ring_send.at[way, far, h], ring_recv.at[way, far, h], right if way == 0 else left)

    x_own = pltpu.make_async_copy(x_ref, x_s.at[core], x_sem.at[0])
    x_mate = to(x_ref, x_s.at[core], x_sem.at[1], x_sem.at[2], mate)

    def needs(r, k, way):
        return r >= k if way == 0 else (r + k >= nz) | (r + k < far)

    def gets(k, way):
        return needs(z, k, way)

    def gives(k, way):
        return needs(lax.rem(z + 1, nz) if way == 0 else lax.rem(z + nz - 1, nz), k, way)

    def half_hop(h, way, part):
        row = pl.ds(pl.multiple_of((core if part == 0 else 1 - core) * own, own), own)
        src, dst = kv_s.at[0, h, :, row], kv_s.at[1 if way == 0 else nz - 1, h, :, row]
        return to(src, dst, half_send.at[way, part, h], half_recv.at[way, part, h], right if way == 0 else left)

    def when(cond, *copies):
        @pl.when(cond)
        def _():
            for act in copies:
                act()

    x_own.start()
    wk_tile(0).start()
    wv_tile(0).start()
    barrier = pltpu.get_barrier_semaphore()
    for device in (mate, left, right):
        pl.semaphore_signal(barrier, inc=1, device_id={"sp": device}, device_id_type=MESH)

    with jax.named_scope("tables"):
        place = lax.broadcasted_iota(jnp.int32, (both, HEAD), 0) + z * both
        angle = place.astype(jnp.float32) * freq_ref[...]
        sign = jnp.where(lax.broadcasted_iota(jnp.int32, (both, HEAD), 1) < HEAD // 2, -1.0, 1.0)
        cos_s[...] = jnp.cos(angle)
        sin_s[...] = jnp.sin(angle) * sign

    with jax.named_scope("barrier"):
        pl.semaphore_wait(barrier, 3)
    x_mate.start()

    def norm(who):
        def chunk(r, _):
            wide = x_s[who, pl.ds(pl.multiple_of(r * 16, 16), 16), :].astype(jnp.float32)
            scale = lax.rsqrt(jnp.mean(wide * wide, -1, keepdims=True) + 1e-6)
            a = (wide * scale * gain_ref[...].astype(jnp.float32).reshape(1, d)).astype(jnp.bfloat16)
            a_s[pl.ds(pl.multiple_of(who * own + r * 16, 16), 16), :] = a

        lax.fori_loop(0, own // 16, chunk, None, unroll=2)

    def turn(t, rows=slice(None)):
        t = t.astype(jnp.bfloat16).astype(jnp.float32)
        return (t * cos_s[rows] + pltpu.roll(t, HEAD // 2, 1) * sin_s[rows]).astype(jnp.bfloat16)

    def keys_of(p, rows):
        got = _dot(a_s[rows], pool[2 * p])
        for i in range(2):
            kv_s[0, 2 * p + i, 0, rows] = turn(got[:, i * HEAD : (i + 1) * HEAD], rows)

    def values_of(p, rows):
        got = _dot(a_s[rows], pool[2 * p + 1]).astype(jnp.bfloat16)
        for i in range(2):
            kv_s[0, 2 * p + i, 1, rows] = got[:, i * HEAD : (i + 1) * HEAD]

    for part in range(2):
        who = core if part == 0 else 1 - core
        here = pl.ds(pl.multiple_of(who * own, own), own)
        with jax.named_scope("norm"):
            if part == 0:
                x_own.wait()
            else:
                x_mate.wait_recv()
            norm(who)
        with jax.named_scope("kv0"):
            if part == 0:
                wk_tile(0).wait()
            keys_of(0, here)
            if part == 0:
                wv_tile(0).wait()
            values_of(0, here)
        for way in range(2):
            when(gives(1, way), *[half_hop(h, way, part).start for h in range(per)])
        if part == 0:
            wk_tile(1).start()
            wv_tile(1).start()
            for i in range(SLOTS - 4):
                wq_tile(i).start()
    for i in range(2):
        wq_tile(SLOTS - 4 + i).start()

    with jax.named_scope("kv1"):
        wk_tile(1).wait()
        keys_of(1, slice(None))
        wv_tile(1).wait()
        values_of(1, slice(None))
    for i in range(2):
        wq_tile(SLOTS - 2 + i).start()

    def start_own(h):
        for way in range(2):
            when(gives(1, way), hop(1, h, way).start)

    start_own(per)

    def queries(i, more):
        wq_tile(i).wait()
        got = _dot(a_s[...], pool[lax.rem(i + groups, SLOTS)])
        for n in range(2):
            q_s[2 * i + n] = turn(got[:, n * HEAD : (n + 1) * HEAD])
        if more:
            wq_tile(i + SLOTS).start()

    with jax.named_scope("qa"):
        lax.fori_loop(0, tiles // 2, lambda i, _: queries(i, True), None)
    for s in range(2):
        for o in range(2):
            wo_tile(s, o).start()

    def attend(j, h, slots, diagonal=False):
        keys = [kv_s[n, h, 0] for n in slots]
        values = jnp.concatenate([kv_s[n, h, 1].T for n in slots], axis=1)
        values = jnp.concatenate([values, jnp.ones((8, values.shape[1]), values.dtype)], axis=0)
        n = STRIP // both
        strips = range(0, g * both, STRIP)
        scores = []
        for at in strips:
            q = q_s[pl.ds(g * h + at // both, n)].reshape(STRIP, HEAD)
            scores.append([_dot(k, q, 1, 1) for k in keys])
        weights, keeps = [], []
        for at, parts in zip(strips, scores):
            if diagonal:
                seen = lax.rem(lax.broadcasted_iota(jnp.int32, (both, STRIP), 1), both) >= lax.broadcasted_iota(jnp.int32, (both, STRIP), 0)
                parts = [jnp.where(seen, parts[0], -jnp.inf)]
            old = None if diagonal else top_s[j, :, at : at + STRIP]
            top = functools.reduce(jnp.maximum, [s.max(axis=0, keepdims=True) for s in parts] + ([] if diagonal else [old]))
            top_s[j, :, at : at + STRIP] = top
            weights.append(jnp.concatenate([jnp.exp2((s - top) * e).astype(jnp.bfloat16) for s in parts], axis=0))
            keeps.append(None if diagonal else jnp.exp2((old - top) * e))
        for at, w, keep in zip(strips, weights, keeps):
            got = _dot(values, w)
            mix_s[j, :, at : at + STRIP] = got if diagonal else mix_s[j, :, at : at + STRIP] * keep + got

    def span(h):
        return slice((h % per) * g * HEAD, (h % per + 1) * g * HEAD)

    def seen(h):
        part = (h // per, slice(None), pl.ds((h % per) * g * HEAD, g * HEAD))
        return to(own_s.at[part], oth_s.at[part], seen_send.at[h], seen_recv.at[h], mate)

    def finish(h):
        j = h % per
        with jax.named_scope("finish"):
            for n in range(g):
                at = slice(n * both, (n + 1) * both)
                out = mix_s[j, :HEAD, at] * (1 / mix_s[j, HEAD : HEAD + 1, at])
                column = (j * g + n) * HEAD
                own_s[h // per, :, column : column + HEAD] = out.T.astype(jnp.bfloat16)
        seen(h).start()

    def stage(s, beside):
        base = s * per

        def arrive(n, _):
            k, j = 1 + lax.div(n, per), lax.rem(n, per)
            h = base + j
            with jax.named_scope("wait"):
                for way in range(2):
                    if s == 0:
                        when(gets(k, way) & (k == 1), *[half_hop(h, way, part).wait_recv for part in range(2)])
                        when(gets(k, way) & (k > 1), hop(k, h, way).wait_recv)
                    else:
                        when(gets(k, way), hop(k, h, way).wait_recv)
            for way in range(2):
                when(gives(k + 1, way) & (k < far - 1), hop(k + 1, h, way).start)
                when(gives(far, way) & (k == far - 1), last_hop(h, way).start)

            with jax.named_scope("diag"):
                @pl.when(k == 1)
                def _():
                    attend(j, h, [0], diagonal=True)

            with jax.named_scope("beside"):
                beside(n)

            with jax.named_scope("att"):
                @pl.when(z + k >= nz)
                def _():
                    attend(j, h, [k, nz - k])

                @pl.when((z + k < nz) & (z >= k))
                def _():
                    attend(j, h, [k])

        lax.fori_loop(0, (far - 1) * per, arrive, None)

    def end(h):
        with jax.named_scope("end"):
            @pl.when(z >= far)
            def _():
                for way in range(2):
                    last_hop(h, way).wait_recv()
                attend(h % per, h, [far])
        finish(h)

    def column_tile(ct):
        return pl.ds(pl.multiple_of(ct * OUT, OUT), OUT)

    def project(h, o, at):
        i = span(h)
        return _dot((own_s, oth_s)[o][h // per, :, i], wo_s[h // per, o, i, at])

    stage(0, lambda n: queries(tiles // 2 + n, False))
    for h in range(per + 1, groups):
        start_own(h)
    for h in range(per):
        end(h)

    for o in range(2):
        wo_tile(0, o).wait()

    def first_half(n):
        @pl.when(n == 0)
        def _():
            for h in range(per):
                seen(h).wait_recv()

        @pl.when(n < half // OUT)
        def _():
            at = column_tile(n)
            acc_s[:, at] = _dot(own_s[0], wo_s[0, 0, :, at]) + _dot(oth_s[0], wo_s[0, 1, :, at])

    stage(1, first_half)

    for o in range(2):
        wo_tile(1, o).wait()

    def passed(work):
        for ct in range(half // OUT):
            work(ct, slice(ct * OUT, (ct + 1) * OUT))

    def own_first(ct, at):
        acc_s[:, at] += project(per, 0, at)

    def own_second(ct, at):
        acc_s[:, at] += project(per + 1, 0, at) + project(per, 1, at)

    def y_mate(ct):
        return to(y_s.at[1 - core, :, pl.ds(ct * OUT, OUT)], y_columns(ct), y_sem.at[0, ct], y_sem.at[1, ct], mate)

    def y_columns(ct):
        return y_ref.at[:, pl.ds(pl.multiple_of(core * half + ct * OUT, OUT), OUT)]

    def mate_second(ct, at):
        total = acc_s[:, at] + project(per + 1, 1, at)
        for i in range(2):
            x = x_s[i, :, pl.ds(pl.multiple_of(core * half + ct * OUT, OUT), OUT)].astype(jnp.float32)
            y_s[i, :, at] = (x + total[i * own : (i + 1) * own]).astype(jnp.bfloat16)
        y_mate(ct).start()

    end(per)
    with jax.named_scope("tail0"):
        passed(own_first)
    end(per + 1)
    seen(per).wait_recv()
    with jax.named_scope("tail1"):
        passed(own_second)
    seen(per + 1).wait_recv()
    with jax.named_scope("tail2"):
        passed(mate_second)
    y_own = pltpu.make_async_copy(y_s.at[core], y_ref.at[:, pl.ds(pl.multiple_of(core * half, OUT), half)], own_sem.at[0])
    y_own.start()

    x_mate.wait_send()
    for h in range(groups):
        seen(h).wait_send()
        for way in range(2):
            if h < per:
                when(gives(1, way), *[half_hop(h, way, part).wait_send for part in range(2)])
            else:
                when(gives(1, way), hop(1, h, way).wait_send)
            for k in range(2, far):
                when(gives(k, way), hop(k, h, way).wait_send)
            when(gives(far, way), last_hop(h, way).wait_send)
    with jax.named_scope("ywait"):
        y_own.wait()
        for ct in range(half // OUT):
            y_mate(ct).wait()


def solution(mesh):
    nz = mesh.shape["sp"] // 2

    def step(x, gain, wq, wk, wv, wo):
        own, d = x.shape
        both = 2 * own
        heads, groups = wq.shape[1] // HEAD // 2, wk.shape[1] // HEAD // 2
        g, per, half = heads // groups, groups // 2, d // 2
        rows = heads * HEAD // 2
        far = nz // 2
        freq = np.float32(THETA) ** (-(np.arange(HEAD) % (HEAD // 2)).astype(np.float32) / (HEAD // 2))
        vmem, hbm = pl.BlockSpec(memory_space=pltpu.VMEM), pl.BlockSpec(memory_space=pl.ANY)
        low = jnp.bfloat16
        dma = pltpu.SemaphoreType.DMA
        return pl.pallas_call(
            functools.partial(_kernel, nz),
            out_shape=jax.ShapeDtypeStruct((own, d), low),
            in_specs=[hbm, vmem, vmem, hbm, hbm, hbm, hbm],
            out_specs=hbm,
            scratch_shapes=[
                pltpu.VMEM((2, own, d), low),
                pltpu.VMEM((both, d), low),
                pltpu.VMEM((SLOTS, d, WIDE), low),
                pltpu.VMEM((2, 2, rows, half), low),
                pltpu.VMEM((nz, groups, 2, both, HEAD), low),
                pltpu.VMEM((heads, both, HEAD), low),
                pltpu.VMEM((per, 1, g * both), jnp.float32),
                pltpu.VMEM((per, HEAD + 8, g * both), jnp.float32),
                pltpu.VMEM((both, half), jnp.float32),
                pltpu.VMEM((2, both, rows), low),
                pltpu.VMEM((2, both, rows), low),
                pltpu.VMEM((2, own, half), low),
                pltpu.VMEM((both, HEAD), jnp.float32),
                pltpu.VMEM((both, HEAD), jnp.float32),
                dma((SLOTS,)),
                dma((2, 2)),
                dma((3,)),
                dma((2, far + 1, groups)),
                dma((2, far + 1, groups)),
                dma((2, 2, groups)),
                dma((2, 2, groups)),
                dma((groups,)),
                dma((groups,)),
                dma((2, d // 2 // OUT)),
                dma((1,)),
            ],
            compiler_params=pltpu.CompilerParams(collective_id=0, has_side_effects=True, vmem_limit_bytes=67043328),
        )(x, gain, jnp.asarray(freq, jnp.float32)[None], wq, wk, wv, wo)

    tokens, whole = P(("dp", "sp"), None), P(None, None)
    return jax.shard_map(
        step,
        mesh=mesh,
        in_specs=(tokens, P(None), whole, whole, whole, whole),
        out_specs=tokens,
        check_vma=False,
    )
```

```python
import functools

import jax
import jax.numpy as jnp
from jax import lax
from jax.experimental import pallas as pl
from jax.experimental.pallas import tpu as pltpu
from jax.sharding import PartitionSpec as P

HEAD = 128
THETA = 10000
LOG2E = 1.4426950408889634
WIDE = 256
SLOTS = 6
STRIP = 512
OUT = 512
MESH = pl.DeviceIdType.MESH


def _dot(a, b, ca=1, cb=0):
    return lax.dot_general(a, b, (((ca,), (cb,)), ((), ())), preferred_element_type=jnp.float32)


def _kernel(nz, x_ref, gain_ref, wq_ref, wk_ref, wv_ref, wo_ref, y_ref, x_s, a_s, pool, wo_s, kv_s, q_s, top_s, mix_s, acc_s, own_s,
            oth_s, y_s, cos_s, sin_s, gain_s, w_sem, wo_sem, x_sem, ring_send, ring_recv, seen_send, seen_recv, y_sem):
    me = lax.axis_index("sp")
    core, z = lax.rem(me, 2), lax.div(me, 2)
    mate = me + 1 - 2 * core
    right, left = 2 * lax.rem(z + 1, nz) + core, 2 * lax.rem(z + nz - 1, nz) + core
    own, d = x_ref.shape
    both = 2 * own
    groups = kv_s.shape[1]
    g = q_s.shape[0] // groups
    per = groups // 2
    rows = own_s.shape[2]
    half = y_s.shape[1]
    far = nz // 2
    tiles = q_s.shape[0] * HEAD // WIDE
    e = HEAD**-0.5 * LOG2E

    def load(ref, column, slot):
        return pltpu.make_async_copy(ref.at[:, pl.ds(pl.multiple_of(column, WIDE), WIDE)], pool.at[slot], w_sem.at[slot])

    def wq_tile(i):
        return load(wq_ref, core * (q_s.shape[0] * HEAD) + i * WIDE, lax.rem(i + 2 * groups // 2, SLOTS))

    def wk_tile(p):
        return load(wk_ref, core * (groups * HEAD) + p * WIDE, 2 * p)

    def wv_tile(p):
        return load(wv_ref, core * (groups * HEAD) + p * WIDE, 2 * p + 1)

    def wo_tile(s, o):
        who = core if o == 0 else 1 - core
        row = pl.multiple_of(who * (2 * rows) + s * rows, 128)
        return pltpu.make_async_copy(wo_ref.at[pl.ds(row, rows), pl.ds(pl.multiple_of(core * half, 128), half)], wo_s.at[s, o], wo_sem.at[s])

    def wo_both(s):
        return pltpu.make_async_copy(wo_s.at[s], wo_s.at[s], wo_sem.at[s])

    def to(src, dst, send, recv, device):
        return pltpu.make_async_remote_copy(src_ref=src, dst_ref=dst, send_sem=send, recv_sem=recv, device_id={"sp": device}, device_id_type=MESH)

    def hop(k, h, way):
        src, dst = (k - 1, k) if way == 0 else (lax.rem(nz + 1 - k, nz), nz - k)
        return to(kv_s.at[src, h], kv_s.at[dst, h], ring_send.at[way, k - 1], ring_recv.at[way, k - 1, h], right if way == 0 else left)

    def last_hop(h, way):
        src = far - 1 if way == 0 else nz + 1 - far
        return to(kv_s.at[src, h, way], kv_s.at[far, h, way], ring_send.at[way, far - 1], ring_recv.at[way, far - 1, h], right if way == 0 else left)

    x_own = pltpu.make_async_copy(x_ref, x_s.at[core], x_sem.at[0])
    x_mate = to(x_ref, x_s.at[core], x_sem.at[1], x_sem.at[2], mate)

    def needs(r, k, way):
        return r >= k if way == 0 else (r + k >= nz) | (r + k < far)

    def gets(k, way):
        return needs(z, k, way)

    def gives(k, way):
        return needs(lax.rem(z + 1, nz) if way == 0 else lax.rem(z + nz - 1, nz), k, way)

    def half_hop(h, way, part):
        row = pl.ds(pl.multiple_of((core if part == 0 else 1 - core) * own, own), own)
        src, dst = kv_s.at[0, h, :, row], kv_s.at[1 if way == 0 else nz - 1, h, :, row]
        return to(src, dst, ring_send.at[way, 0], ring_recv.at[way, 0, h], right if way == 0 else left)

    def when(cond, *copies):
        @pl.when(cond)
        def _():
            for act in copies:
                act()

    gain = pltpu.make_async_copy(gain_ref, gain_s, x_sem.at[3])
    x_own.start()
    gain.start()
    barrier = pltpu.get_barrier_semaphore()
    for device in (mate, left, right):
        pl.semaphore_signal(barrier, inc=1, device_id={"sp": device}, device_id_type=MESH)

    with jax.named_scope("tables"):
        place = lax.broadcasted_iota(jnp.int32, (both, HEAD), 0) + z * both
        lane = lax.broadcasted_iota(jnp.int32, (1, HEAD), 1)
        freq = jnp.ones((1, HEAD), jnp.float32)
        for bit in range((HEAD // 2).bit_length() - 1):
            freq = jnp.where(lax.rem(lax.div(lane, 2**bit), 2) == 1, freq * THETA ** (-(2**bit) / (HEAD // 2)), freq)
        angle = place.astype(jnp.float32) * freq
        sign = jnp.where(lane < HEAD // 2, -1.0, 1.0)
        cos_s[...] = jnp.cos(angle)
        sin_s[...] = jnp.sin(angle) * sign

    wk_tile(0).start()
    wv_tile(0).start()
    with jax.named_scope("barrier"):
        pl.semaphore_wait(barrier, 3)
    x_mate.start()

    def norm(who):
        def chunk(r, _):
            wide = x_s[who, pl.ds(pl.multiple_of(r * 16, 16), 16), :].astype(jnp.float32)
            scale = lax.rsqrt(jnp.mean(wide * wide, -1, keepdims=True) + 1e-6)
            a = (wide * scale * gain_s[...].astype(jnp.float32).reshape(1, d)).astype(jnp.bfloat16)
            a_s[pl.ds(pl.multiple_of(who * own + r * 16, 16), 16), :] = a

        lax.fori_loop(0, own // 16, chunk, None, unroll=2)

    def turn(t, rows=slice(None)):
        t = t.astype(jnp.bfloat16).astype(jnp.float32)
        return (t * cos_s[rows] + pltpu.roll(t, HEAD // 2, 1) * sin_s[rows]).astype(jnp.bfloat16)

    def keys_of(p, rows):
        got = _dot(a_s[rows], pool[2 * p])
        for i in range(2):
            kv_s[0, 2 * p + i, 0, rows] = turn(got[:, i * HEAD : (i + 1) * HEAD], rows)

    def values_of(p, rows):
        got = _dot(a_s[rows], pool[2 * p + 1]).astype(jnp.bfloat16)
        for i in range(2):
            kv_s[0, 2 * p + i, 1, rows] = got[:, i * HEAD : (i + 1) * HEAD]

    for part in range(2):
        who = core if part == 0 else 1 - core
        here = pl.ds(pl.multiple_of(who * own, own), own)
        with jax.named_scope("norm"):
            if part == 0:
                x_own.wait()
                gain.wait()
                wk_tile(1).start()
                wv_tile(1).start()
            else:
                x_mate.wait_recv()
            norm(who)
        with jax.named_scope("kv0"):
            if part == 0:
                wk_tile(0).wait()
            keys_of(0, here)
            if part == 0:
                wv_tile(0).wait()
            values_of(0, here)
        for way in range(2):
            when(gives(1, way), *[half_hop(h, way, part).start for h in range(per)])
        for i in range(2):
            wq_tile(2 * part + i).start()

    with jax.named_scope("kv1"):
        wk_tile(1).wait()
        keys_of(1, slice(None))
        wv_tile(1).wait()
        values_of(1, slice(None))
    for i in range(2):
        wq_tile(SLOTS - 2 + i).start()

    def start_own(h):
        for way in range(2):
            when(gives(1, way), hop(1, h, way).start)

    start_own(per)

    def queries(i, more):
        wq_tile(i).wait()
        got = _dot(a_s[...], pool[lax.rem(i + groups, SLOTS)])
        for n in range(2):
            q_s[2 * i + n] = turn(got[:, n * HEAD : (n + 1) * HEAD])
        if more:
            wq_tile(i + SLOTS).start()

    with jax.named_scope("qa"):
        lax.fori_loop(0, tiles // 2, lambda i, _: queries(i, True), None)
    for s in range(2):
        for o in range(2):
            wo_tile(s, o).start()

    def attend(j, h, slots, diagonal=False):
        keys = [kv_s[n, h, 0] for n in slots]
        values = jnp.concatenate([kv_s[n, h, 1].T for n in slots], axis=1)
        values = jnp.concatenate([values, jnp.ones((8, values.shape[1]), values.dtype)], axis=0)
        n = STRIP // both
        strips = range(0, g * both, STRIP)
        scores = []
        for at in strips:
            q = q_s[pl.ds(g * h + at // both, n)].reshape(STRIP, HEAD)
            scores.append([_dot(k, q, 1, 1) for k in keys])
        weights, keeps = [], []
        for at, parts in zip(strips, scores):
            if diagonal:
                seen = lax.rem(lax.broadcasted_iota(jnp.int32, (both, STRIP), 1), both) >= lax.broadcasted_iota(jnp.int32, (both, STRIP), 0)
                parts = [jnp.where(seen, parts[0], -jnp.inf)]
            old = None if diagonal else top_s[j, :, at : at + STRIP]
            top = functools.reduce(jnp.maximum, [s.max(axis=0, keepdims=True) for s in parts] + ([] if diagonal else [old]))
            top_s[j, :, at : at + STRIP] = top
            weights.append(jnp.concatenate([jnp.exp2((s - top) * e).astype(jnp.bfloat16) for s in parts], axis=0))
            keeps.append(None if diagonal else jnp.exp2((old - top) * e))
        for at, w, keep in zip(strips, weights, keeps):
            got = _dot(values, w)
            mix_s[j, :, at : at + STRIP] = got if diagonal else mix_s[j, :, at : at + STRIP] * keep + got

    def span(h):
        return slice((h % per) * g * HEAD, (h % per + 1) * g * HEAD)

    def seen(h):
        part = (h // per, slice(None), pl.ds((h % per) * g * HEAD, g * HEAD))
        return to(own_s.at[part], oth_s.at[part], seen_send.at[0], seen_recv.at[max(h - per + 1, 0)], mate)

    def seen_all(s):
        return to(own_s.at[s], oth_s.at[s], seen_send.at[0], seen_recv.at[0], mate)

    def finish(h):
        j = h % per
        with jax.named_scope("finish"):
            for n in range(g):
                at = slice(n * both, (n + 1) * both)
                out = mix_s[j, :HEAD, at] * (1 / mix_s[j, HEAD : HEAD + 1, at])
                column = (j * g + n) * HEAD
                own_s[h // per, :, column : column + HEAD] = out.T.astype(jnp.bfloat16)
        seen(h).start()

    def stage(s, beside):
        base = s * per

        def arrive(n, _):
            k, j = 1 + lax.div(n, per), lax.rem(n, per)
            h = base + j
            early = s > 0

            with jax.named_scope("wait"):
                for way in range(2):
                    when(gets(k, way) & (n > 0) if early else gets(k, way), hop(k, h, way).wait_recv)
            for way in range(2):
                when(gives(k + 1, way) & ((k < far - 1) & (n > 0) if early else k < far - 1), hop(k + 1, h, way).start)
                when(gives(far, way) & (k == far - 1), last_hop(h, way).start)
            if s == 0:
                @pl.when(n == (far - 1) * per - 1)
                def _():
                    for later in range(per + 1, groups):
                        start_own(later)
                    for way in range(2):
                        when(gets(1, way), hop(1, per, way).wait_recv)
                        when(gives(2, way), hop(2, per, way).start)

            with jax.named_scope("diag"):
                @pl.when(k == 1)
                def _():
                    attend(j, h, [0], diagonal=True)

            with jax.named_scope("beside"):
                beside(n)

            with jax.named_scope("att"):
                @pl.when(z + k >= nz)
                def _():
                    attend(j, h, [k, nz - k])

                @pl.when((z + k < nz) & (z >= k))
                def _():
                    attend(j, h, [k])

        lax.fori_loop(0, (far - 1) * per, arrive, None)

    def end(h):
        with jax.named_scope("end"):
            @pl.when(z >= far)
            def _():
                for way in range(2):
                    last_hop(h, way).wait_recv()
                attend(h % per, h, [far])
        finish(h)

    def column_tile(ct):
        return pl.ds(pl.multiple_of(ct * OUT, OUT), OUT)

    def project(h, o, at):
        i = span(h)
        return _dot((own_s, oth_s)[o][h // per, :, i], wo_s[h // per, o, i, at])

    stage(0, lambda n: queries(tiles // 2 + n, False))
    for h in range(per):
        end(h)

    wo_both(0).wait()

    def first_half(n):
        @pl.when(n == 0)
        def _():
            seen_all(0).wait_recv()

        @pl.when(n < half // OUT)
        def _():
            at = column_tile(n)
            acc_s[:, at] = _dot(own_s[0], wo_s[0, 0, :, at]) + _dot(oth_s[0], wo_s[0, 1, :, at])
            for i in range(2):
                x = x_s[i, :, pl.ds(pl.multiple_of(core * half + n * OUT, OUT), OUT)].astype(jnp.float32)
                acc_s[i * own : (i + 1) * own, at] += x

    stage(1, first_half)

    wo_both(1).wait()

    def passed(work):
        for ct in range(half // OUT):
            work(ct, slice(ct * OUT, (ct + 1) * OUT))

    def own_first(ct, at):
        acc_s[:, at] += project(per, 0, at)

    def own_second(ct, at):
        acc_s[:, at] += project(per + 1, 0, at) + project(per, 1, at)

    def columns(width, at=0):
        return pl.ds(pl.multiple_of(core * half + at, OUT), width)

    def y_mate(width, at=0):
        return to(y_s.at[:, pl.ds(at, width)], y_ref.at[:, columns(width, at)], y_sem.at[0], y_sem.at[1], mate)

    def mate_second(ct, at):
        acc_s[:, at] += project(per + 1, 1, at)
        y_s[:, at] = acc_s[pl.ds(pl.multiple_of((1 - core) * own, own), own), at].astype(jnp.bfloat16)
        y_mate(OUT, ct * OUT).start()
        y_ref[:, columns(OUT, ct * OUT)] = acc_s[pl.ds(pl.multiple_of(core * own, own), own), at].astype(jnp.bfloat16)

    end(per)
    with jax.named_scope("tail0"):
        passed(own_first)
    end(per + 1)
    seen(per).wait_recv()
    with jax.named_scope("tail1"):
        passed(own_second)
    seen(per + 1).wait_recv()
    with jax.named_scope("tail2"):
        passed(mate_second)
    with jax.named_scope("sent"):
        x_mate.wait_send()
        to(own_s, oth_s, seen_send.at[0], seen_recv.at[0], mate).wait_send()
        for way in range(2):
            for k in range(1, far):
                when(gives(k, way), to(kv_s.at[0], kv_s.at[1], ring_send.at[way, k - 1], ring_recv.at[way, k - 1, 0], mate).wait_send)
            last = to(kv_s.at[0, :, way], kv_s.at[1, :, way], ring_send.at[way, far - 1], ring_recv.at[way, far - 1, 0], mate)
            when(gives(far, way), last.wait_send)
    with jax.named_scope("ywait"):
        y_mate(half).wait()


def solution(mesh):
    nz = mesh.shape["sp"] // 2

    def step(x, gain, wq, wk, wv, wo):
        own, d = x.shape
        both = 2 * own
        heads, groups = wq.shape[1] // HEAD // 2, wk.shape[1] // HEAD // 2
        g, per, half = heads // groups, groups // 2, d // 2
        rows = heads * HEAD // 2
        far = nz // 2
        hbm = pl.BlockSpec(memory_space=pl.ANY)
        low = jnp.bfloat16
        dma = pltpu.SemaphoreType.DMA
        return pl.pallas_call(
            functools.partial(_kernel, nz),
            out_shape=pltpu.VMEM((own, d), low),
            in_specs=[hbm] * 6,
            out_specs=pl.BlockSpec(memory_space=pltpu.VMEM),
            scratch_shapes=[
                pltpu.VMEM((2, own, d), low),
                pltpu.VMEM((both, d), low),
                pltpu.VMEM((SLOTS, d, WIDE), low),
                pltpu.VMEM((2, 2, rows, half), low),
                pltpu.VMEM((nz, groups, 2, both, HEAD), low),
                pltpu.VMEM((heads, both, HEAD), low),
                pltpu.VMEM((per, 1, g * both), jnp.float32),
                pltpu.VMEM((per, HEAD + 8, g * both), jnp.float32),
                pltpu.VMEM((both, half), jnp.float32),
                pltpu.VMEM((2, both, rows), low),
                pltpu.VMEM((2, both, rows), low),
                pltpu.VMEM((own, half), low),
                pltpu.VMEM((both, HEAD), jnp.float32),
                pltpu.VMEM((both, HEAD), jnp.float32),
                pltpu.VMEM((d,), low),
                dma((SLOTS,)),
                dma((2,)),
                dma((4,)),
                dma((2, far)),
                dma((2, far, groups)),
                dma((1,)),
                dma((1 + groups - per,)),
                dma((2,)),
            ],
            compiler_params=pltpu.CompilerParams(collective_id=0, has_side_effects=True, vmem_limit_bytes=62 * 2**20),
        )(x, gain, wq, wk, wv, wo)

    tokens, whole = P(("dp", "sp"), None), P(None, None)
    return jax.shard_map(
        step,
        mesh=mesh,
        in_specs=(tokens, P(None), whole, whole, whole, whole),
        out_specs=tokens,
        check_vma=False,
    )
```

```python
import functools

import jax
import jax.numpy as jnp
from jax import lax
from jax.experimental import pallas as pl
from jax.experimental.pallas import tpu as pltpu
from jax.sharding import PartitionSpec as P

HEAD = 128
THETA = 10000
LOG2E = 1.4426950408889634
WIDE = 256
SLOTS = 6
STRIP = 512
OUT = 512
MESH = pl.DeviceIdType.MESH


def _dot(a, b, ca=1, cb=0):
    return lax.dot_general(a, b, (((ca,), (cb,)), ((), ())), preferred_element_type=jnp.float32)


def _kernel(nz, x_ref, gain_ref, wq_ref, wk_ref, wv_ref, wo_ref, y_ref, x_s, a_s, pool, wo_s, kv_s, qa_s, qb_s, top_s, mix_s, acc_s, own_s,
            oth_s, y_s, cos_s, sin_s, gain_s, w_sem, wo_sem, x_sem, ring_send, ring_recv, rest_recv, seen_send, seen_recv, y_sem):
    me = lax.axis_index("sp")
    core, z = lax.rem(me, 2), lax.div(me, 2)
    mate = me + 1 - 2 * core
    right, left = 2 * lax.rem(z + 1, nz) + core, 2 * lax.rem(z + nz - 1, nz) + core
    own, d = x_ref.shape
    both = 2 * own
    groups = kv_s.shape[1]
    per = groups // 2
    g = qa_s.shape[0] // per
    rows = own_s.shape[2]
    half = y_s.shape[1]
    far = nz // 2
    tiles = groups * g * HEAD // WIDE
    e = HEAD**-0.5 * LOG2E

    def load(ref, column, slot):
        return pltpu.make_async_copy(ref.at[:, pl.ds(pl.multiple_of(column, WIDE), WIDE)], pool.at[slot], w_sem.at[slot])

    def wq_tile(i):
        return load(wq_ref, core * (groups * g * HEAD) + i * WIDE, lax.rem(i + 2 * groups // 2, SLOTS))

    def wk_tile(p):
        return load(wk_ref, core * (groups * HEAD) + p * WIDE, 2 * p)

    def wv_tile(p):
        return load(wv_ref, core * (groups * HEAD) + p * WIDE, 2 * p + 1)

    def wo_tile(s, o):
        who = core if o == 0 else 1 - core
        row = pl.multiple_of(who * (2 * rows) + s * rows, 128)
        return pltpu.make_async_copy(wo_ref.at[pl.ds(row, rows), pl.ds(pl.multiple_of(core * half, 128), half)], wo_s.at[s, o], wo_sem.at[s])

    def wo_both(s):
        return pltpu.make_async_copy(wo_s.at[s], wo_s.at[s], wo_sem.at[s])

    def to(src, dst, send, recv, device):
        return pltpu.make_async_remote_copy(src_ref=src, dst_ref=dst, send_sem=send, recv_sem=recv, device_id={"sp": device}, device_id_type=MESH)

    def hop(k, h, way):
        src, dst = (k - 1, k) if way == 0 else (lax.rem(nz + 1 - k, nz), nz - k)
        return to(kv_s.at[src, h], kv_s.at[dst, h], ring_send.at[way, k - 1], ring_recv.at[way, k - 1, h], right if way == 0 else left)

    def part_hop(h, way, i):
        k = far - 1
        src, dst = (k - 1, k) if way == 0 else (nz + 1 - k, nz - k)
        recv = (ring_recv if i == way else rest_recv).at[(way, k - 1, h) if i == way else (way, h)]
        return to(kv_s.at[src, h, i], kv_s.at[dst, h, i], ring_send.at[way, k - 1], recv, right if way == 0 else left)

    def last_hop(h, way):
        src = far - 1 if way == 0 else nz + 1 - far
        return to(kv_s.at[src, h, way], kv_s.at[far, h, way], ring_send.at[way, far - 1], ring_recv.at[way, far - 1, h], right if way == 0 else left)

    x_own = pltpu.make_async_copy(x_ref, x_s.at[core], x_sem.at[0])
    x_mate = to(x_ref, x_s.at[core], x_sem.at[1], x_sem.at[2], mate)

    def needs(r, k, way):
        return r >= k if way == 0 else (r + k >= nz) | (r + k < far)

    def gets(k, way):
        return needs(z, k, way)

    def gives(k, way):
        return needs(lax.rem(z + 1, nz) if way == 0 else lax.rem(z + nz - 1, nz), k, way)

    def half_hop(h, way, part):
        row = pl.ds(pl.multiple_of((core if part == 0 else 1 - core) * own, own), own)
        src, dst = kv_s.at[0, h, :, row], kv_s.at[1 if way == 0 else nz - 1, h, :, row]
        return to(src, dst, ring_send.at[way, 0], ring_recv.at[way, 0, h], right if way == 0 else left)

    def when(cond, *copies):
        @pl.when(cond)
        def _():
            for act in copies:
                act()

    gain = pltpu.make_async_copy(gain_ref, gain_s, x_sem.at[3])
    x_own.start()
    gain.start()
    barrier = pltpu.get_barrier_semaphore()
    for device in (mate, left, right):
        pl.semaphore_signal(barrier, inc=1, device_id={"sp": device}, device_id_type=MESH)

    with jax.named_scope("tables"):
        place = lax.broadcasted_iota(jnp.int32, (both, HEAD), 0) + z * both
        lane = lax.broadcasted_iota(jnp.int32, (1, HEAD), 1)
        freq = jnp.ones((1, HEAD), jnp.float32)
        for bit in range((HEAD // 2).bit_length() - 1):
            freq = jnp.where(lax.rem(lax.div(lane, 2**bit), 2) == 1, freq * THETA ** (-(2**bit) / (HEAD // 2)), freq)
        angle = place.astype(jnp.float32) * freq
        sign = jnp.where(lane < HEAD // 2, -1.0, 1.0)
        cos_s[...] = jnp.cos(angle)
        wk_tile(0).start()
        wv_tile(0).start()
        sin_s[...] = jnp.sin(angle) * sign

    def meet():
        with jax.named_scope("barrier"):
            pl.semaphore_wait(barrier, 3)
        x_mate.start()

    when(z >= far, meet)

    def norm(who):
        def chunk(r, _):
            wide = x_s[who, pl.ds(pl.multiple_of(r * 16, 16), 16), :].astype(jnp.float32)
            scale = lax.rsqrt(jnp.mean(wide * wide, -1, keepdims=True) + 1e-6)
            a = (wide * scale * gain_s[...].astype(jnp.float32).reshape(1, d)).astype(jnp.bfloat16)
            a_s[pl.ds(pl.multiple_of(who * own + r * 16, 16), 16), :] = a

        lax.fori_loop(0, own // 16, chunk, None, unroll=2)

    def turn(t, rows=slice(None)):
        t = t.astype(jnp.bfloat16).astype(jnp.float32)
        return (t * cos_s[rows] + pltpu.roll(t, HEAD // 2, 1) * sin_s[rows]).astype(jnp.bfloat16)

    def keys_values(p, here, first):
        if first:
            wk_tile(p).wait()
            wv_tile(p).wait()
        a = a_s[here]
        keys, values = _dot(a, pool[2 * p]), _dot(a, pool[2 * p + 1]).astype(jnp.bfloat16)
        for i in range(2):
            at = slice(i * HEAD, (i + 1) * HEAD)
            kv_s[0, 2 * p + i, 0, here] = turn(keys[:, at], here)
            kv_s[0, 2 * p + i, 1, here] = values[:, at]

    for part in range(2):
        who = core if part == 0 else 1 - core
        here = pl.ds(pl.multiple_of(who * own, own), own)
        with jax.named_scope("norm"):
            if part == 0:
                x_own.wait()
                gain.wait()
            else:
                x_mate.wait_recv()
            norm(who)
        if part == 0:
            wk_tile(1).start()
            wv_tile(1).start()
        with jax.named_scope("kv0"):
            keys_values(0, here, part == 0)
        if part == 0:
            when(z < far, meet)
        for way in range(2):
            when(gives(1, way), *[half_hop(h, way, part).start for h in range(per)])
        for i in range(2):
            wq_tile(2 * part + i).start()
        with jax.named_scope("kv1"):
            keys_values(1, here, part == 0)
    for i in range(2):
        wq_tile(SLOTS - 2 + i).start()

    def start_own(h):
        for way in range(2):
            when(gives(1, way), hop(1, h, way).start)

    start_own(per)

    def queries(ref, i, tile):
        got = _dot(a_s[...], pool[lax.rem(tile + groups, SLOTS)])
        for n in range(2):
            ref[2 * i + n] = turn(got[:, n * HEAD : (n + 1) * HEAD])

    def forward(k, h):
        for way in range(2):
            more = gives(k + 1, way)
            when(more & (k + 1 < far - 1), hop(k + 1, h, way).start)
            when(more & (k + 1 == far - 1), part_hop(h, way, way).start, part_hop(h, way, 1 - way).start)
            when(more & (k + 1 == far), last_hop(h, way).start)

    def arrived(k, h):
        with jax.named_scope("wait"):
            for way in range(2):
                when(gets(k, way) & (k < far - 1), hop(k, h, way).wait_recv)
                when(gets(k, way) & (k == far - 1), part_hop(h, way, way).wait_recv)
        forward(k, h)

    def first_queries(i, _):
        for n in range(2):
            wq_tile(2 * i + n).wait()
        for n in range(2):
            queries(qa_s, 2 * i + n, 2 * i + n)
        for n in range(2):
            wq_tile(2 * i + n + SLOTS).start()
        for j in range(per):
            when(i == 1 + j, lambda: arrived(1, j))

    with jax.named_scope("qa"):
        lax.fori_loop(0, tiles // 4, first_queries, None)
    for s in range(2):
        for o in range(2):
            wo_tile(s, o).start()

    def attend(q_s, j, h, slots, diagonal=False, beside=None):
        keys = [kv_s[n, h, 0] for n in slots]
        values = jnp.concatenate([kv_s[n, h, 1].T for n in slots], axis=1)
        values = jnp.concatenate([values, jnp.ones((8, values.shape[1]), values.dtype)], axis=0)
        n = STRIP // both
        strips = range(0, g * both, STRIP)
        scores = []
        for at in strips:
            q = q_s[pl.ds(g * j + at // both, n)].reshape(STRIP, HEAD)
            scores.append([_dot(k, q, 1, 1) for k in keys])
        if beside is not None:
            beside()
        weights, keeps = [], []
        for at, parts in zip(strips, scores):
            if diagonal:
                seen = lax.rem(lax.broadcasted_iota(jnp.int32, (both, STRIP), 1), both) >= lax.broadcasted_iota(jnp.int32, (both, STRIP), 0)
                parts = [jnp.where(seen, parts[0], -jnp.inf)]
            old = None if diagonal else top_s[j, :, at : at + STRIP]
            top = functools.reduce(jnp.maximum, [s.max(axis=0, keepdims=True) for s in parts] + ([] if diagonal else [old]))
            top_s[j, :, at : at + STRIP] = top
            weights.append(jnp.concatenate([jnp.exp2((s - top) * e).astype(jnp.bfloat16) for s in parts], axis=0))
            keeps.append(None if diagonal else jnp.exp2((old - top) * e))
        for at, w, keep in zip(strips, weights, keeps):
            got = _dot(values, w)
            mix_s[j, :, at : at + STRIP] = got if diagonal else mix_s[j, :, at : at + STRIP] * keep + got

    def span(h):
        return slice((h % per) * g * HEAD, (h % per + 1) * g * HEAD)

    def seen(h):
        part = (h // per, slice(None), pl.ds((h % per) * g * HEAD, g * HEAD))
        return to(own_s.at[part], oth_s.at[part], seen_send.at[0], seen_recv.at[max(h - per + 1, 0)], mate)

    def seen_all(s):
        return to(own_s.at[s], oth_s.at[s], seen_send.at[0], seen_recv.at[0], mate)

    def finish(h):
        j = h % per
        with jax.named_scope("finish"):
            for n in range(g):
                at = slice(n * both, (n + 1) * both)
                out = mix_s[j, :HEAD, at] * (1 / mix_s[j, HEAD : HEAD + 1, at])
                column = (j * g + n) * HEAD
                own_s[h // per, :, column : column + HEAD] = out.T.astype(jnp.bfloat16)
        seen(h).start()

    def stage(s, steps, ready, beside):
        base = s * per
        q_s = (qa_s, qb_s)[s]

        def arrive(n, _):
            k, j = 1 + lax.div(n, per), lax.rem(n, per)
            h = base + j
            if s > 0:
                when(n == 1, *[lambda: arrived(1, base + i) for i in range(1, per)])
            when(n >= per, lambda: arrived(k, h))
            if s == 0:
                @pl.when(n == (far - 1) * per - 1)
                def _():
                    for later in range(per + 1, groups):
                        start_own(later)
                    arrived(1, per)

            with jax.named_scope("diag"):
                @pl.when(k == 1)
                def _():
                    attend(q_s, j, h, [0], diagonal=True)

            ready(n)
            with jax.named_scope("rest"):
                for way in range(2):
                    when(gets(k, way) & (k == far - 1), part_hop(h, way, 1 - way).wait_recv)

            def work(busy):
                todo = (lambda: beside(n)) if busy else None
                with jax.named_scope("att"):
                    @pl.when(z + k >= nz)
                    def _():
                        attend(q_s, j, h, [k, nz - k], beside=todo)

                    @pl.when((z + k < nz) & (z >= k))
                    def _():
                        attend(q_s, j, h, [k], beside=todo)

                    if busy:
                        when(z < k, todo)

            if steps == (far - 1) * per:
                work(True)
            else:
                when(n < steps, lambda: work(True))
                when(n >= steps, lambda: work(False))

        lax.fori_loop(0, (far - 1) * per, arrive, None)

    def end(h):
        q_s = (qa_s, qb_s)[h // per]
        with jax.named_scope("end"):
            @pl.when(z >= far)
            def _():
                for way in range(2):
                    last_hop(h, way).wait_recv()
                attend(q_s, h % per, h, [far])
        finish(h)

    def column_tile(ct):
        return pl.ds(pl.multiple_of(ct * OUT, OUT), OUT)

    def project(h, o, at):
        i = span(h)
        return _dot((own_s, oth_s)[o][h // per, :, i], wo_s[h // per, o, i, at])

    stage(0, tiles // 2, lambda n: wq_tile(tiles // 2 + n).wait(), lambda n: queries(qb_s, n, tiles // 2 + n))
    for h in range(per):
        end(h)

    wo_both(0).wait()

    def first_half(n):
        at = column_tile(n)
        acc_s[:, at] = _dot(own_s[0], wo_s[0, 0, :, at]) + _dot(oth_s[0], wo_s[0, 1, :, at])
        for i in range(2):
            x = x_s[i, :, pl.ds(pl.multiple_of(core * half + n * OUT, OUT), OUT)].astype(jnp.float32)
            acc_s[i * own : (i + 1) * own, at] += x

    stage(1, half // OUT, lambda n: when(n == 0, seen_all(0).wait_recv), first_half)

    wo_both(1).wait()

    def passed(work):
        for ct in range(half // OUT):
            work(ct, slice(ct * OUT, (ct + 1) * OUT))

    def own_first(ct, at):
        acc_s[:, at] += project(per, 0, at)

    def own_second(ct, at):
        acc_s[:, at] += project(per + 1, 0, at) + project(per, 1, at)

    def columns(width, at=0):
        return pl.ds(pl.multiple_of(core * half + at, OUT), width)

    def y_mate(width, at=0):
        return to(y_s.at[:, pl.ds(at, width)], y_ref.at[:, columns(width, at)], y_sem.at[0], y_sem.at[1], mate)

    def last(who, at):
        here = pl.ds(pl.multiple_of(who * own, own), own)
        i = span(per + 1)
        return (acc_s[here, at] + _dot(oth_s[1, here, i], wo_s[1, 1, i, at])).astype(jnp.bfloat16)

    def mate_rows(ct, at):
        y_s[:, at] = last(1 - core, at)
        y_mate(OUT, ct * OUT).start()

    def own_rows(ct, at):
        y_ref[:, columns(OUT, ct * OUT)] = last(core, at)

    end(per)
    with jax.named_scope("tail0"):
        passed(own_first)
    end(per + 1)
    seen(per).wait_recv()
    with jax.named_scope("tail1"):
        passed(own_second)
    seen(per + 1).wait_recv()
    with jax.named_scope("tail2"):
        passed(mate_rows)
        passed(own_rows)
    with jax.named_scope("sent"):
        x_mate.wait_send()
        to(own_s, oth_s, seen_send.at[0], seen_recv.at[0], mate).wait_send()
        for way in range(2):
            for k in range(1, far):
                when(gives(k, way), to(kv_s.at[0], kv_s.at[1], ring_send.at[way, k - 1], ring_recv.at[way, k - 1, 0], mate).wait_send)
            last = to(kv_s.at[0, :, way], kv_s.at[1, :, way], ring_send.at[way, far - 1], ring_recv.at[way, far - 1, 0], mate)
            when(gives(far, way), last.wait_send)
    with jax.named_scope("ywait"):
        y_mate(half).wait()


def solution(mesh):
    nz = mesh.shape["sp"] // 2

    def step(x, gain, wq, wk, wv, wo):
        own, d = x.shape
        both = 2 * own
        heads, groups = wq.shape[1] // HEAD // 2, wk.shape[1] // HEAD // 2
        g, per, half = heads // groups, groups // 2, d // 2
        rows = heads * HEAD // 2
        far = nz // 2
        hbm = pl.BlockSpec(memory_space=pl.ANY)
        low = jnp.bfloat16
        dma = pltpu.SemaphoreType.DMA
        return pl.pallas_call(
            functools.partial(_kernel, nz),
            out_shape=pltpu.VMEM((own, d), low),
            in_specs=[hbm] * 6,
            out_specs=pl.BlockSpec(memory_space=pltpu.VMEM),
            scratch_shapes=[
                pltpu.VMEM((2, own, d), low),
                pltpu.VMEM((both, d), low),
                pltpu.VMEM((SLOTS, d, WIDE), low),
                pltpu.VMEM((2, 2, rows, half), low),
                pltpu.VMEM((nz, groups, 2, both, HEAD), low),
                pltpu.VMEM((heads // 2, both, HEAD), low),
                pltpu.VMEM((heads // 2, both, HEAD), low),
                pltpu.VMEM((per, 1, g * both), jnp.float32),
                pltpu.VMEM((per, HEAD + 8, g * both), jnp.float32),
                pltpu.VMEM((both, half), jnp.float32),
                pltpu.VMEM((2, both, rows), low),
                pltpu.VMEM((2, both, rows), low),
                pltpu.VMEM((own, half), low),
                pltpu.VMEM((both, HEAD), jnp.float32),
                pltpu.VMEM((both, HEAD), jnp.float32),
                pltpu.VMEM((d,), low),
                dma((SLOTS,)),
                dma((2,)),
                dma((4,)),
                dma((2, far)),
                dma((2, far, groups)),
                dma((2, groups)),
                dma((1,)),
                dma((1 + groups - per,)),
                dma((2,)),
            ],
            compiler_params=pltpu.CompilerParams(collective_id=0, has_side_effects=True, vmem_limit_bytes=62 * 2**20),
        )(x, gain, wq, wk, wv, wo)

    tokens, whole = P(("dp", "sp"), None), P(None, None)
    return jax.shard_map(
        step,
        mesh=mesh,
        in_specs=(tokens, P(None), whole, whole, whole, whole),
        out_specs=tokens,
        check_vma=False,
    )
```

```python
import functools

import jax
import jax.numpy as jnp
from jax import lax
from jax.experimental import pallas as pl
from jax.experimental.pallas import tpu as pltpu
from jax.sharding import PartitionSpec as P

HEAD = 128
THETA = 10000
LOG2E = 1.4426950408889634
WIDE = 256
SLOTS = 6
STRIP = 512
OUT = 512
LAST = 1024
MESH = pl.DeviceIdType.MESH


def _dot(a, b, ca=1, cb=0):
    return lax.dot_general(a, b, (((ca,), (cb,)), ((), ())), preferred_element_type=jnp.float32)


def _kernel(nz, x_ref, gain_ref, wq_ref, wk_ref, wv_ref, wo_ref, y_ref, x_s, a_s, pool, wo_s, kv_s, qa_s, qb_s, top_s, mix_s, acc_s, own_s,
            oth_s, y_s, cos_s, sin_s, gain_s, w_sem, wo_sem, x_sem, ring_send, ring_recv, rest_recv, seen_send, seen_recv, y_sem):
    me = lax.axis_index("sp")
    core, z = lax.rem(me, 2), lax.div(me, 2)
    mate = me + 1 - 2 * core
    right, left = 2 * lax.rem(z + 1, nz) + core, 2 * lax.rem(z + nz - 1, nz) + core
    own, d = x_ref.shape
    both = 2 * own
    groups = kv_s.shape[1]
    per = groups // 2
    g = qa_s.shape[0] // per
    rows = own_s.shape[2]
    half = y_s.shape[1]
    far = nz // 2
    tiles = groups * g * HEAD // WIDE
    e = HEAD**-0.5 * LOG2E

    def load(ref, column, slot):
        return pltpu.make_async_copy(ref.at[:, pl.ds(pl.multiple_of(column, WIDE), WIDE)], pool.at[slot], w_sem.at[slot])

    def wq_tile(i):
        return load(wq_ref, core * (groups * g * HEAD) + i * WIDE, lax.rem(i + 2 * groups // 2, SLOTS))

    def wk_tile(p):
        return load(wk_ref, core * (groups * HEAD) + p * WIDE, 2 * p)

    def wv_tile(p):
        return load(wv_ref, core * (groups * HEAD) + p * WIDE, 2 * p + 1)

    def wo_tile(s, o):
        who = core if o == 0 else 1 - core
        row = pl.multiple_of(who * (2 * rows) + s * rows, 128)
        return pltpu.make_async_copy(wo_ref.at[pl.ds(row, rows), pl.ds(pl.multiple_of(core * half, 128), half)], wo_s.at[s, o], wo_sem.at[s])

    def wo_both(s):
        return pltpu.make_async_copy(wo_s.at[s], wo_s.at[s], wo_sem.at[s])

    def to(src, dst, send, recv, device):
        return pltpu.make_async_remote_copy(src_ref=src, dst_ref=dst, send_sem=send, recv_sem=recv, device_id={"sp": device}, device_id_type=MESH)

    def hop(k, h, way):
        src, dst = (k - 1, k) if way == 0 else (lax.rem(nz + 1 - k, nz), nz - k)
        return to(kv_s.at[src, h], kv_s.at[dst, h], ring_send.at[way, k - 1], ring_recv.at[way, k - 1, h], right if way == 0 else left)

    def part_hop(h, way, i):
        k = far - 1
        src, dst = (k - 1, k) if way == 0 else (nz + 1 - k, nz - k)
        recv = (ring_recv if i == way else rest_recv).at[(way, k - 1, h) if i == way else (way, h)]
        return to(kv_s.at[src, h, i], kv_s.at[dst, h, i], ring_send.at[way, k - 1], recv, right if way == 0 else left)

    def last_hop(h, way):
        src = far - 1 if way == 0 else nz + 1 - far
        return to(kv_s.at[src, h, way], kv_s.at[far, h, way], ring_send.at[way, far - 1], ring_recv.at[way, far - 1, h], right if way == 0 else left)

    x_own = pltpu.make_async_copy(x_ref, x_s.at[core], x_sem.at[0])
    x_mate = to(x_ref, x_s.at[core], x_sem.at[1], x_sem.at[2], mate)

    def needs(r, k, way):
        return r >= k if way == 0 else (r + k >= nz) | (r + k < far)

    def gets(k, way):
        return needs(z, k, way)

    def gives(k, way):
        return needs(lax.rem(z + 1, nz) if way == 0 else lax.rem(z + nz - 1, nz), k, way)

    def half_hop(h, way, part):
        row = pl.ds(pl.multiple_of((core if part == 0 else 1 - core) * own, own), own)
        src, dst = kv_s.at[0, h, :, row], kv_s.at[1 if way == 0 else nz - 1, h, :, row]
        return to(src, dst, ring_send.at[way, 0], ring_recv.at[way, 0, h], right if way == 0 else left)

    def when(cond, *copies):
        @pl.when(cond)
        def _():
            for act in copies:
                act()

    gain = pltpu.make_async_copy(gain_ref, gain_s, x_sem.at[3])
    x_own.start()
    gain.start()
    wk_tile(0).start()
    wv_tile(0).start()
    barrier = pltpu.get_barrier_semaphore()
    for device in (mate, left, right):
        pl.semaphore_signal(barrier, inc=1, device_id={"sp": device}, device_id_type=MESH)

    with jax.named_scope("tables"):
        place = lax.broadcasted_iota(jnp.int32, (both, HEAD), 0) + z * both
        lane = lax.broadcasted_iota(jnp.int32, (1, HEAD), 1)
        freq = jnp.ones((1, HEAD), jnp.float32)
        for bit in range((HEAD // 2).bit_length() - 1):
            freq = jnp.where(lax.rem(lax.div(lane, 2**bit), 2) == 1, freq * THETA ** (-(2**bit) / (HEAD // 2)), freq)
        angle = place.astype(jnp.float32) * freq
        sign = jnp.where(lane < HEAD // 2, -1.0, 1.0)
        cos_s[...] = jnp.cos(angle)
        sin_s[...] = jnp.sin(angle) * sign

    def meet():
        with jax.named_scope("barrier"):
            pl.semaphore_wait(barrier, 3)
        x_mate.start()

    when(z >= far, meet)

    def norm(who):
        def chunk(r, _):
            wide = x_s[who, pl.ds(pl.multiple_of(r * 16, 16), 16), :].astype(jnp.float32)
            scale = lax.rsqrt(jnp.mean(wide * wide, -1, keepdims=True) + 1e-6)
            a = (wide * scale * gain_s[...].astype(jnp.float32).reshape(1, d)).astype(jnp.bfloat16)
            a_s[pl.ds(pl.multiple_of(who * own + r * 16, 16), 16), :] = a

        lax.fori_loop(0, own // 16, chunk, None, unroll=8)

    def turn(t, rows=slice(None)):
        t = t.astype(jnp.bfloat16).astype(jnp.float32)
        return (t * cos_s[rows] + pltpu.roll(t, HEAD // 2, 1) * sin_s[rows]).astype(jnp.bfloat16)

    def keys_values(p, here, first):
        if first:
            wk_tile(p).wait()
            wv_tile(p).wait()
        a = a_s[here]
        keys, values = _dot(a, pool[2 * p]), _dot(a, pool[2 * p + 1]).astype(jnp.bfloat16)
        for i in range(2):
            at = slice(i * HEAD, (i + 1) * HEAD)
            kv_s[0, 2 * p + i, 0, here] = turn(keys[:, at], here)
            kv_s[0, 2 * p + i, 1, here] = values[:, at]

    for part in range(2):
        who = core if part == 0 else 1 - core
        here = pl.ds(pl.multiple_of(who * own, own), own)
        with jax.named_scope("norm"):
            if part == 0:
                x_own.wait()
                gain.wait()
            else:
                x_mate.wait_recv()
            norm(who)
        if part == 0:
            wk_tile(1).start()
            wv_tile(1).start()
        with jax.named_scope("kv0"):
            keys_values(0, here, part == 0)
        if part == 0:
            when(z < far, meet)
        for way in range(2):
            when(gives(1, way), *[half_hop(h, way, part).start for h in range(per)])
        for i in range(2):
            wq_tile(2 * part + i).start()
    with jax.named_scope("kv1"):
        for part in range(2):
            who = core if part == 0 else 1 - core
            keys_values(1, pl.ds(pl.multiple_of(who * own, own), own), part == 0)
    for i in range(2):
        wq_tile(SLOTS - 2 + i).start()

    def start_own(h):
        for way in range(2):
            when(gives(1, way), hop(1, h, way).start)

    start_own(per)

    def queries(ref, i, tile):
        got = _dot(a_s[...], pool[lax.rem(tile + groups, SLOTS)])
        for n in range(2):
            ref[2 * i + n] = turn(got[:, n * HEAD : (n + 1) * HEAD])

    def forward(k, h):
        for way in range(2):
            more = gives(k + 1, way)
            when(more & (k + 1 < far - 1), hop(k + 1, h, way).start)
            when(more & (k + 1 == far - 1), part_hop(h, way, way).start, part_hop(h, way, 1 - way).start)
            when(more & (k + 1 == far), last_hop(h, way).start)

    def arrived(k, h):
        with jax.named_scope("wait"):
            for way in range(2):
                when(gets(k, way) & (k < far - 1), hop(k, h, way).wait_recv)
                when(gets(k, way) & (k == far - 1), part_hop(h, way, way).wait_recv)
        forward(k, h)

    def first_queries(i, _):
        for n in range(2):
            wq_tile(2 * i + n).wait()
        for n in range(2):
            queries(qa_s, 2 * i + n, 2 * i + n)
        for n in range(2):
            wq_tile(2 * i + n + SLOTS).start()
        for j in range(per):
            when(i == 1 + j, lambda: arrived(1, j))

    with jax.named_scope("qa"):
        lax.fori_loop(0, tiles // 4, first_queries, None)
    for s in range(2):
        for o in range(2):
            wo_tile(s, o).start()

    def attend(q_s, j, h, slots, diagonal=False, beside=None):
        keys = [kv_s[n, h, 0] for n in slots]
        values = jnp.concatenate([kv_s[n, h, 1].T for n in slots], axis=1)
        values = jnp.concatenate([values, jnp.ones((8, values.shape[1]), values.dtype)], axis=0)
        n = STRIP // both
        strips = range(0, g * both, STRIP)
        scores = []
        for at in strips:
            q = q_s[pl.ds(g * j + at // both, n)].reshape(STRIP, HEAD)
            scores.append([_dot(k, q, 1, 1) for k in keys])
        if beside is not None:
            beside()
        weights, keeps = [], []
        for at, parts in zip(strips, scores):
            if diagonal:
                seen = lax.rem(lax.broadcasted_iota(jnp.int32, (both, STRIP), 1), both) >= lax.broadcasted_iota(jnp.int32, (both, STRIP), 0)
                parts = [jnp.where(seen, parts[0], -jnp.inf)]
            old = None if diagonal else top_s[j, :, at : at + STRIP]
            top = functools.reduce(jnp.maximum, [s.max(axis=0, keepdims=True) for s in parts] + ([] if diagonal else [old]))
            top_s[j, :, at : at + STRIP] = top
            weights.append(jnp.concatenate([jnp.exp2((s - top) * e).astype(jnp.bfloat16) for s in parts], axis=0))
            keeps.append(None if diagonal else jnp.exp2((old - top) * e))
        for at, w, keep in zip(strips, weights, keeps):
            got = _dot(values, w)
            mix_s[j, :, at : at + STRIP] = got if diagonal else mix_s[j, :, at : at + STRIP] * keep + got

    def span(h):
        return slice((h % per) * g * HEAD, (h % per + 1) * g * HEAD)

    def seen(h):
        part = (h // per, slice(None), pl.ds((h % per) * g * HEAD, g * HEAD))
        return to(own_s.at[part], oth_s.at[part], seen_send.at[0], seen_recv.at[max(h - per + 1, 0)], mate)

    def seen_all(s):
        return to(own_s.at[s], oth_s.at[s], seen_send.at[0], seen_recv.at[0], mate)

    def finish(h):
        j = h % per
        with jax.named_scope("finish"):
            for n in range(g):
                at = slice(n * both, (n + 1) * both)
                out = mix_s[j, :HEAD, at] * (1 / mix_s[j, HEAD : HEAD + 1, at])
                column = (j * g + n) * HEAD
                own_s[h // per, :, column : column + HEAD] = out.T.astype(jnp.bfloat16)
        seen(h).start()

    def stage(s, begin, steps, ready, beside):
        base = s * per
        q_s = (qa_s, qb_s)[s]

        def arrive(n, _):
            k, j = 1 + lax.div(n, per), lax.rem(n, per)
            h = base + j
            if s > 0:
                when(n == 1, *[lambda: arrived(1, base + i) for i in range(1, per)])
            when(n >= per, lambda: arrived(k, h))
            if s == 0:
                @pl.when(n == (far - 1) * per - 1)
                def _():
                    for later in range(per + 1, groups):
                        start_own(later)
                    arrived(1, per)

            with jax.named_scope("diag"):
                @pl.when(k == 1)
                def _():
                    attend(q_s, j, h, [0], diagonal=True)

            ready(n - begin)
            with jax.named_scope("rest"):
                for way in range(2):
                    when(gets(k, way) & (k == far - 1), part_hop(h, way, 1 - way).wait_recv)

            def work(busy):
                todo = (lambda: beside(n - begin)) if busy else None
                with jax.named_scope("att"):
                    @pl.when(z + k >= nz)
                    def _():
                        attend(q_s, j, h, [k, nz - k], beside=todo)

                    @pl.when((z + k < nz) & (z >= k))
                    def _():
                        attend(q_s, j, h, [k], beside=todo)

                    if busy:
                        when(z < k, todo)

            if steps == (far - 1) * per:
                work(True)
            else:
                busy = (n >= begin) & (n < begin + steps)
                when(busy, lambda: work(True))
                when(jnp.logical_not(busy), lambda: work(False))

        lax.fori_loop(0, (far - 1) * per, arrive, None)

    def end(h):
        q_s = (qa_s, qb_s)[h // per]
        with jax.named_scope("end"):
            @pl.when(z >= far)
            def _():
                for way in range(2):
                    last_hop(h, way).wait_recv()
                attend(q_s, h % per, h, [far])
        finish(h)

    def column_tile(ct):
        return pl.ds(pl.multiple_of(ct * OUT, OUT), OUT)

    def project(h, o, at):
        i = span(h)
        return _dot((own_s, oth_s)[o][h // per, :, i], wo_s[h // per, o, i, at])

    stage(0, 0, tiles // 2, lambda n: wq_tile(tiles // 2 + n).wait(), lambda n: queries(qb_s, n, tiles // 2 + n))
    for h in range(per):
        end(h)

    wo_both(0).wait()

    def first_half(n):
        at = column_tile(n)
        acc_s[:, at] = _dot(own_s[0], wo_s[0, 0, :, at]) + _dot(oth_s[0], wo_s[0, 1, :, at])
        for i in range(2):
            x = x_s[i, :, pl.ds(pl.multiple_of(core * half + n * OUT, OUT), OUT)].astype(jnp.float32)
            acc_s[i * own : (i + 1) * own, at] += x

    stage(1, 1, half // OUT, lambda n: when(n == 0, seen_all(0).wait_recv), first_half)

    wo_both(1).wait()

    def passed(work, width=OUT):
        for ct in range(half // width):
            work(ct, slice(ct * width, (ct + 1) * width))

    def own_first(ct, at):
        acc_s[:, at] += project(per, 0, at)

    def own_second(ct, at):
        acc_s[:, at] += project(per + 1, 0, at) + project(per, 1, at)

    def columns(width, at=0):
        return pl.ds(pl.multiple_of(core * half + at, OUT), width)

    def y_mate(width, at=0):
        return to(y_s.at[:, pl.ds(at, width)], y_ref.at[:, columns(width, at)], y_sem.at[0], y_sem.at[1], mate)

    def last(who, at):
        here = pl.ds(pl.multiple_of(who * own, own), own)
        i = span(per + 1)
        return (acc_s[here, at] + _dot(oth_s[1, here, i], wo_s[1, 1, i, at])).astype(jnp.bfloat16)

    def mate_rows(ct, at):
        y_s[:, at] = last(1 - core, at)
        y_mate(LAST, ct * LAST).start()

    def own_rows(ct, at):
        y_ref[:, columns(LAST, ct * LAST)] = last(core, at)

    end(per)
    with jax.named_scope("tail0"):
        passed(own_first)
    end(per + 1)
    seen(per).wait_recv()
    with jax.named_scope("tail1"):
        passed(own_second)
    seen(per + 1).wait_recv()
    with jax.named_scope("tail2"):
        passed(mate_rows, LAST)
        passed(own_rows, LAST)
    with jax.named_scope("sent"):
        x_mate.wait_send()
        to(own_s, oth_s, seen_send.at[0], seen_recv.at[0], mate).wait_send()
        for way in range(2):
            for k in range(1, far):
                when(gives(k, way), to(kv_s.at[0], kv_s.at[1], ring_send.at[way, k - 1], ring_recv.at[way, k - 1, 0], mate).wait_send)
            last = to(kv_s.at[0, :, way], kv_s.at[1, :, way], ring_send.at[way, far - 1], ring_recv.at[way, far - 1, 0], mate)
            when(gives(far, way), last.wait_send)
    with jax.named_scope("ywait"):
        y_mate(half).wait()


def solution(mesh):
    nz = mesh.shape["sp"] // 2

    def step(x, gain, wq, wk, wv, wo):
        own, d = x.shape
        both = 2 * own
        heads, groups = wq.shape[1] // HEAD // 2, wk.shape[1] // HEAD // 2
        g, per, half = heads // groups, groups // 2, d // 2
        rows = heads * HEAD // 2
        far = nz // 2
        hbm = pl.BlockSpec(memory_space=pl.ANY)
        low = jnp.bfloat16
        dma = pltpu.SemaphoreType.DMA
        return pl.pallas_call(
            functools.partial(_kernel, nz),
            out_shape=pltpu.VMEM((own, d), low),
            in_specs=[hbm] * 6,
            out_specs=pl.BlockSpec(memory_space=pltpu.VMEM),
            scratch_shapes=[
                pltpu.VMEM((2, own, d), low),
                pltpu.VMEM((both, d), low),
                pltpu.VMEM((SLOTS, d, WIDE), low),
                pltpu.VMEM((2, 2, rows, half), low),
                pltpu.VMEM((nz, groups, 2, both, HEAD), low),
                pltpu.VMEM((heads // 2, both, HEAD), low),
                pltpu.VMEM((heads // 2, both, HEAD), low),
                pltpu.VMEM((per, 1, g * both), jnp.float32),
                pltpu.VMEM((per, HEAD + 8, g * both), jnp.float32),
                pltpu.VMEM((both, half), jnp.float32),
                pltpu.VMEM((2, both, rows), low),
                pltpu.VMEM((2, both, rows), low),
                pltpu.VMEM((own, half), low),
                pltpu.VMEM((both, HEAD), jnp.float32),
                pltpu.VMEM((both, HEAD), jnp.float32),
                pltpu.VMEM((d,), low),
                dma((SLOTS,)),
                dma((2,)),
                dma((4,)),
                dma((2, far)),
                dma((2, far, groups)),
                dma((2, groups)),
                dma((1,)),
                dma((1 + groups - per,)),
                dma((2,)),
            ],
            compiler_params=pltpu.CompilerParams(collective_id=0, has_side_effects=True, vmem_limit_bytes=62 * 2**20),
        )(x, gain, wq, wk, wv, wo)

    tokens, whole = P(("dp", "sp"), None), P(None, None)
    return jax.shard_map(
        step,
        mesh=mesh,
        in_specs=(tokens, P(None), whole, whole, whole, whole),
        out_specs=tokens,
        check_vma=False,
    )
```

```python
import functools

import jax
import jax.numpy as jnp
from jax import lax
from jax.experimental import pallas as pl
from jax.experimental.pallas import tpu as pltpu
from jax.sharding import PartitionSpec as P

HEAD = 128
THETA = 10000
LOG2E = 1.4426950408889634
WIDE = 256
SLOTS = 6
STRIP = 512
OUT = 512
LAST = 1024
MESH = pl.DeviceIdType.MESH


def _dot(a, b, ca=1, cb=0):
    return lax.dot_general(a, b, (((ca,), (cb,)), ((), ())), preferred_element_type=jnp.float32)


def _kernel(nz, x_ref, gain_ref, wq_ref, wk_ref, wv_ref, wo_ref, y_ref, x_s, a_s, pool, wo_s, kv_s, qa_s, qb_s, top_s, mix_s, acc_s, own_s,
            oth_s, y_s, cos_s, sin_s, gain_s, w_sem, wo_sem, x_sem, ring_send, ring_recv, rest_recv, seen_send, seen_recv, y_sem):
    me = lax.axis_index("sp")
    core, z = lax.rem(me, 2), lax.div(me, 2)
    mate = me + 1 - 2 * core
    right, left = 2 * lax.rem(z + 1, nz) + core, 2 * lax.rem(z + nz - 1, nz) + core
    own, d = x_ref.shape
    both = 2 * own
    groups = kv_s.shape[1]
    per = groups // 2
    g = qa_s.shape[0] // per
    rows = own_s.shape[2]
    half = y_s.shape[1]
    far = nz // 2
    tiles = groups * g * HEAD // WIDE
    e = HEAD**-0.5 * LOG2E

    def load(ref, column, slot):
        return pltpu.make_async_copy(ref.at[:, pl.ds(pl.multiple_of(column, WIDE), WIDE)], pool.at[slot], w_sem.at[slot])

    def wq_tile(i):
        return load(wq_ref, core * (groups * g * HEAD) + i * WIDE, lax.rem(i + 2 * groups // 2, SLOTS))

    def wk_tile(p):
        return load(wk_ref, core * (groups * HEAD) + p * WIDE, 2 * p)

    def wv_tile(p):
        return load(wv_ref, core * (groups * HEAD) + p * WIDE, 2 * p + 1)

    def first_head(h, i):
        column = pl.ds(pl.multiple_of(core * (groups * HEAD) + h * HEAD, HEAD), HEAD)
        slot = i if h == 0 else groups + i
        return pltpu.make_async_copy((wk_ref, wv_ref)[i].at[:, column], pool.at[i, :, pl.ds(h * HEAD, HEAD)], w_sem.at[slot])

    def wo_tile(s, o):
        who = core if o == 0 else 1 - core
        row = pl.multiple_of(who * (2 * rows) + s * rows, 128)
        return pltpu.make_async_copy(wo_ref.at[pl.ds(row, rows), pl.ds(pl.multiple_of(core * half, 128), half)], wo_s.at[s, o], wo_sem.at[s])

    def wo_both(s):
        return pltpu.make_async_copy(wo_s.at[s], wo_s.at[s], wo_sem.at[s])

    def to(src, dst, send, recv, device):
        return pltpu.make_async_remote_copy(src_ref=src, dst_ref=dst, send_sem=send, recv_sem=recv, device_id={"sp": device}, device_id_type=MESH)

    def hop(k, h, way):
        src, dst = (k - 1, k) if way == 0 else (lax.rem(nz + 1 - k, nz), nz - k)
        return to(kv_s.at[src, h], kv_s.at[dst, h], ring_send.at[way, k - 1], ring_recv.at[way, k - 1, h], right if way == 0 else left)

    def part_hop(h, way, i):
        k = far - 1
        src, dst = (k - 1, k) if way == 0 else (nz + 1 - k, nz - k)
        recv = (ring_recv if i == way else rest_recv).at[(way, k - 1, h) if i == way else (way, h)]
        return to(kv_s.at[src, h, i], kv_s.at[dst, h, i], ring_send.at[way, k - 1], recv, right if way == 0 else left)

    def last_hop(h, way):
        src = far - 1 if way == 0 else nz + 1 - far
        return to(kv_s.at[src, h, way], kv_s.at[far, h, way], ring_send.at[way, far - 1], ring_recv.at[way, far - 1, h], right if way == 0 else left)

    x_own = pltpu.make_async_copy(x_ref, x_s.at[core], x_sem.at[0])
    x_mate = to(x_ref, x_s.at[core], x_sem.at[1], x_sem.at[2], mate)

    def needs(r, k, way):
        return r >= k if way == 0 else (r + k >= nz) | (r + k < far)

    def gets(k, way):
        return needs(z, k, way)

    def gives(k, way):
        return needs(lax.rem(z + 1, nz) if way == 0 else lax.rem(z + nz - 1, nz), k, way)

    def half_hop(h, way, part):
        row = pl.ds(pl.multiple_of((core if part == 0 else 1 - core) * own, own), own)
        src, dst = kv_s.at[0, h, :, row], kv_s.at[1 if way == 0 else nz - 1, h, :, row]
        return to(src, dst, ring_send.at[way, 0], ring_recv.at[way, 0, h], right if way == 0 else left)

    def when(cond, *copies):
        @pl.when(cond)
        def _():
            for act in copies:
                act()

    gain = pltpu.make_async_copy(gain_ref, gain_s, x_sem.at[3])
    x_own.start()
    gain.start()
    for i in range(2):
        first_head(0, i).start()
    barrier = pltpu.get_barrier_semaphore()
    for device in (mate, left, right):
        pl.semaphore_signal(barrier, inc=1, device_id={"sp": device}, device_id_type=MESH)

    with jax.named_scope("tables"):
        place = lax.broadcasted_iota(jnp.int32, (both, HEAD), 0) + z * both
        lane = lax.broadcasted_iota(jnp.int32, (1, HEAD), 1)
        freq = jnp.ones((1, HEAD), jnp.float32)
        for bit in range((HEAD // 2).bit_length() - 1):
            freq = jnp.where(lax.rem(lax.div(lane, 2**bit), 2) == 1, freq * THETA ** (-(2**bit) / (HEAD // 2)), freq)
        angle = place.astype(jnp.float32) * freq
        sign = jnp.where(lane < HEAD // 2, -1.0, 1.0)
        cos_s[...] = jnp.cos(angle)
        for i in range(2):
            first_head(1, i).start()
        sin_s[...] = jnp.sin(angle) * sign

    def meet():
        with jax.named_scope("barrier"):
            pl.semaphore_wait(barrier, 3)
        x_mate.start()

    when(z >= far, meet)

    def norm(who):
        def chunk(r, _):
            wide = x_s[who, pl.ds(pl.multiple_of(r * 16, 16), 16), :].astype(jnp.float32)
            scale = lax.rsqrt(jnp.mean(wide * wide, -1, keepdims=True) + 1e-6)
            a = (wide * scale * gain_s[...].astype(jnp.float32).reshape(1, d)).astype(jnp.bfloat16)
            a_s[pl.ds(pl.multiple_of(who * own + r * 16, 16), 16), :] = a

        lax.fori_loop(0, own // 16, chunk, None, unroll=8)

    def turn(t, rows=slice(None)):
        t = t.astype(jnp.bfloat16).astype(jnp.float32)
        return (t * cos_s[rows] + pltpu.roll(t, HEAD // 2, 1) * sin_s[rows]).astype(jnp.bfloat16)

    def keys_values(p, here, first):
        if first:
            wk_tile(p).wait()
            wv_tile(p).wait()
        a = a_s[here]
        keys, values = _dot(a, pool[2 * p]), _dot(a, pool[2 * p + 1]).astype(jnp.bfloat16)
        for i in range(2):
            at = slice(i * HEAD, (i + 1) * HEAD)
            kv_s[0, 2 * p + i, 0, here] = turn(keys[:, at], here)
            kv_s[0, 2 * p + i, 1, here] = values[:, at]

    for part in range(2):
        who = core if part == 0 else 1 - core
        here = pl.ds(pl.multiple_of(who * own, own), own)
        with jax.named_scope("norm"):
            if part == 0:
                x_own.wait()
                gain.wait()
            else:
                x_mate.wait_recv()
            norm(who)
        if part == 0:
            wk_tile(1).start()
            wv_tile(1).start()
        with jax.named_scope("kv0"):
            if part == 0:
                for h in range(per):
                    for i in range(2):
                        first_head(h, i).wait()
                    at = slice(h * HEAD, (h + 1) * HEAD)
                    a = a_s[here]
                    keys, values = _dot(a, pool[0, :, at]), _dot(a, pool[1, :, at])
                    kv_s[0, h, 0, here] = turn(keys, here)
                    kv_s[0, h, 1, here] = values.astype(jnp.bfloat16)
                    if h == 0:
                        when(z < far, meet)
                    for way in range(2):
                        when(gives(1, way), half_hop(h, way, part).start)
            else:
                keys_values(0, here, False)
                for way in range(2):
                    when(gives(1, way), *[half_hop(h, way, part).start for h in range(per)])
        for i in range(2):
            wq_tile(2 * part + i).start()
    with jax.named_scope("kv1"):
        for part in range(2):
            who = core if part == 0 else 1 - core
            keys_values(1, pl.ds(pl.multiple_of(who * own, own), own), part == 0)
    for i in range(2):
        wq_tile(SLOTS - 2 + i).start()

    def start_own(h):
        for way in range(2):
            when(gives(1, way), hop(1, h, way).start)

    start_own(per)

    def queries(ref, i, tile):
        got = _dot(a_s[...], pool[lax.rem(tile + groups, SLOTS)])
        for n in range(2):
            ref[2 * i + n] = turn(got[:, n * HEAD : (n + 1) * HEAD])

    def forward(k, h):
        for way in range(2):
            more = gives(k + 1, way)
            when(more & (k + 1 < far - 1), hop(k + 1, h, way).start)
            when(more & (k + 1 == far - 1), part_hop(h, way, way).start, part_hop(h, way, 1 - way).start)
            when(more & (k + 1 == far), last_hop(h, way).start)

    def arrived(k, h):
        with jax.named_scope("wait"):
            for way in range(2):
                when(gets(k, way) & (k < far - 1), hop(k, h, way).wait_recv)
                when(gets(k, way) & (k == far - 1), part_hop(h, way, way).wait_recv)
        forward(k, h)

    def first_queries(i, _):
        for n in range(2):
            wq_tile(2 * i + n).wait()
        for n in range(2):
            queries(qa_s, 2 * i + n, 2 * i + n)
        for n in range(2):
            wq_tile(2 * i + n + SLOTS).start()
        for j in range(per):
            when(i == 1 + j, lambda: arrived(1, j))

    with jax.named_scope("qa"):
        lax.fori_loop(0, tiles // 4, first_queries, None)
    for s in range(2):
        for o in range(2):
            wo_tile(s, o).start()

    def attend(q_s, j, h, slots, diagonal=False, beside=None):
        keys = [kv_s[n, h, 0] for n in slots]
        values = jnp.concatenate([kv_s[n, h, 1].T for n in slots], axis=1)
        values = jnp.concatenate([values, jnp.ones((8, values.shape[1]), values.dtype)], axis=0)
        n = STRIP // both
        strips = range(0, g * both, STRIP)
        scores = []
        for at in strips:
            q = q_s[pl.ds(g * j + at // both, n)].reshape(STRIP, HEAD)
            scores.append([_dot(k, q, 1, 1) for k in keys])
        if beside is not None:
            beside()
        weights, keeps = [], []
        for at, parts in zip(strips, scores):
            if diagonal:
                seen = lax.rem(lax.broadcasted_iota(jnp.int32, (both, STRIP), 1), both) >= lax.broadcasted_iota(jnp.int32, (both, STRIP), 0)
                parts = [jnp.where(seen, parts[0], -jnp.inf)]
            old = None if diagonal else top_s[j, :, at : at + STRIP]
            top = functools.reduce(jnp.maximum, [s.max(axis=0, keepdims=True) for s in parts] + ([] if diagonal else [old]))
            top_s[j, :, at : at + STRIP] = top
            weights.append(jnp.concatenate([jnp.exp2((s - top) * e).astype(jnp.bfloat16) for s in parts], axis=0))
            keeps.append(None if diagonal else jnp.exp2((old - top) * e))
        for at, w, keep in zip(strips, weights, keeps):
            got = _dot(values, w)
            mix_s[j, :, at : at + STRIP] = got if diagonal else mix_s[j, :, at : at + STRIP] * keep + got

    def span(h):
        return slice((h % per) * g * HEAD, (h % per + 1) * g * HEAD)

    def seen(h):
        part = (h // per, slice(None), pl.ds((h % per) * g * HEAD, g * HEAD))
        return to(own_s.at[part], oth_s.at[part], seen_send.at[0], seen_recv.at[max(h - per + 1, 0)], mate)

    def seen_all(s):
        return to(own_s.at[s], oth_s.at[s], seen_send.at[0], seen_recv.at[0], mate)

    def finish(h):
        j = h % per
        with jax.named_scope("finish"):
            for n in range(g):
                at = slice(n * both, (n + 1) * both)
                out = mix_s[j, :HEAD, at] * (1 / mix_s[j, HEAD : HEAD + 1, at])
                column = (j * g + n) * HEAD
                own_s[h // per, :, column : column + HEAD] = out.T.astype(jnp.bfloat16)
        seen(h).start()

    def stage(s, begin, steps, ready, beside):
        base = s * per
        q_s = (qa_s, qb_s)[s]

        def arrive(n, _):
            k, j = 1 + lax.div(n, per), lax.rem(n, per)
            h = base + j
            if s > 0:
                when(n == 1, *[lambda: arrived(1, base + i) for i in range(1, per)])
            when(n >= per, lambda: arrived(k, h))
            if s == 0:
                @pl.when(n == (far - 1) * per - 1)
                def _():
                    for later in range(per + 1, groups):
                        start_own(later)
                    arrived(1, per)

            with jax.named_scope("diag"):
                @pl.when(k == 1)
                def _():
                    attend(q_s, j, h, [0], diagonal=True)

            ready(n - begin)
            with jax.named_scope("rest"):
                for way in range(2):
                    when(gets(k, way) & (k == far - 1), part_hop(h, way, 1 - way).wait_recv)

            def work(busy):
                todo = (lambda: beside(n - begin)) if busy else None
                with jax.named_scope("att"):
                    @pl.when(z + k >= nz)
                    def _():
                        attend(q_s, j, h, [k, nz - k], beside=todo)

                    @pl.when((z + k < nz) & (z >= k))
                    def _():
                        attend(q_s, j, h, [k], beside=todo)

                    if busy:
                        when(z < k, todo)

            if steps == (far - 1) * per:
                work(True)
            else:
                busy = (n >= begin) & (n < begin + steps)
                when(busy, lambda: work(True))
                when(jnp.logical_not(busy), lambda: work(False))

        lax.fori_loop(0, (far - 1) * per, arrive, None)

    def end(h):
        q_s = (qa_s, qb_s)[h // per]
        with jax.named_scope("end"):
            @pl.when(z >= far)
            def _():
                for way in range(2):
                    last_hop(h, way).wait_recv()
                attend(q_s, h % per, h, [far])
        finish(h)

    def column_tile(ct):
        return pl.ds(pl.multiple_of(ct * OUT, OUT), OUT)

    def project(h, o, at):
        i = span(h)
        return _dot((own_s, oth_s)[o][h // per, :, i], wo_s[h // per, o, i, at])

    stage(0, 0, tiles // 2, lambda n: wq_tile(tiles // 2 + n).wait(), lambda n: queries(qb_s, n, tiles // 2 + n))
    for h in range(per):
        end(h)

    wo_both(0).wait()

    def first_half(n):
        at = column_tile(n)
        acc_s[:, at] = _dot(own_s[0], wo_s[0, 0, :, at]) + _dot(oth_s[0], wo_s[0, 1, :, at])
        for i in range(2):
            x = x_s[i, :, pl.ds(pl.multiple_of(core * half + n * OUT, OUT), OUT)].astype(jnp.float32)
            acc_s[i * own : (i + 1) * own, at] += x

    stage(1, 1, half // OUT, lambda n: when(n == 0, seen_all(0).wait_recv), first_half)

    wo_both(1).wait()

    def passed(work, width=OUT):
        for ct in range(half // width):
            work(ct, slice(ct * width, (ct + 1) * width))

    def own_first(ct, at):
        acc_s[:, at] += project(per, 0, at)

    def own_second(ct, at):
        acc_s[:, at] += project(per + 1, 0, at) + project(per, 1, at)

    def columns(width, at=0):
        return pl.ds(pl.multiple_of(core * half + at, OUT), width)

    def y_mate(width, at=0):
        return to(y_s.at[:, pl.ds(at, width)], y_ref.at[:, columns(width, at)], y_sem.at[0], y_sem.at[1], mate)

    def last(who, at):
        here = pl.ds(pl.multiple_of(who * own, own), own)
        i = span(per + 1)
        return (acc_s[here, at] + _dot(oth_s[1, here, i], wo_s[1, 1, i, at])).astype(jnp.bfloat16)

    def mate_rows(ct, at):
        y_s[:, at] = last(1 - core, at)
        y_mate(LAST, ct * LAST).start()

    def own_rows(ct, at):
        y_ref[:, columns(LAST, ct * LAST)] = last(core, at)

    end(per)
    with jax.named_scope("tail0"):
        passed(own_first)
    end(per + 1)
    seen(per).wait_recv()
    with jax.named_scope("tail1"):
        passed(own_second)
    seen(per + 1).wait_recv()
    with jax.named_scope("tail2"):
        passed(mate_rows, LAST)
        passed(own_rows, LAST)
    with jax.named_scope("sent"):
        x_mate.wait_send()
        to(own_s, oth_s, seen_send.at[0], seen_recv.at[0], mate).wait_send()
        for way in range(2):
            for k in range(1, far):
                when(gives(k, way), to(kv_s.at[0], kv_s.at[1], ring_send.at[way, k - 1], ring_recv.at[way, k - 1, 0], mate).wait_send)
            last = to(kv_s.at[0, :, way], kv_s.at[1, :, way], ring_send.at[way, far - 1], ring_recv.at[way, far - 1, 0], mate)
            when(gives(far, way), last.wait_send)
    with jax.named_scope("ywait"):
        y_mate(half).wait()


def solution(mesh):
    nz = mesh.shape["sp"] // 2

    def step(x, gain, wq, wk, wv, wo):
        own, d = x.shape
        both = 2 * own
        heads, groups = wq.shape[1] // HEAD // 2, wk.shape[1] // HEAD // 2
        g, per, half = heads // groups, groups // 2, d // 2
        rows = heads * HEAD // 2
        far = nz // 2
        hbm = pl.BlockSpec(memory_space=pl.ANY)
        low = jnp.bfloat16
        dma = pltpu.SemaphoreType.DMA
        return pl.pallas_call(
            functools.partial(_kernel, nz),
            out_shape=pltpu.VMEM((own, d), low),
            in_specs=[hbm] * 6,
            out_specs=pl.BlockSpec(memory_space=pltpu.VMEM),
            scratch_shapes=[
                pltpu.VMEM((2, own, d), low),
                pltpu.VMEM((both, d), low),
                pltpu.VMEM((SLOTS, d, WIDE), low),
                pltpu.VMEM((2, 2, rows, half), low),
                pltpu.VMEM((nz, groups, 2, both, HEAD), low),
                pltpu.VMEM((heads // 2, both, HEAD), low),
                pltpu.VMEM((heads // 2, both, HEAD), low),
                pltpu.VMEM((per, 1, g * both), jnp.float32),
                pltpu.VMEM((per, HEAD + 8, g * both), jnp.float32),
                pltpu.VMEM((both, half), jnp.float32),
                pltpu.VMEM((2, both, rows), low),
                pltpu.VMEM((2, both, rows), low),
                pltpu.VMEM((own, half), low),
                pltpu.VMEM((both, HEAD), jnp.float32),
                pltpu.VMEM((both, HEAD), jnp.float32),
                pltpu.VMEM((d,), low),
                dma((SLOTS,)),
                dma((2,)),
                dma((4,)),
                dma((2, far)),
                dma((2, far, groups)),
                dma((2, groups)),
                dma((1,)),
                dma((1 + groups - per,)),
                dma((2,)),
            ],
            compiler_params=pltpu.CompilerParams(collective_id=0, has_side_effects=True, vmem_limit_bytes=62 * 2**20),
        )(x, gain, wq, wk, wv, wo)

    tokens, whole = P(("dp", "sp"), None), P(None, None)
    return jax.shard_map(
        step,
        mesh=mesh,
        in_specs=(tokens, P(None), whole, whole, whole, whole),
        out_specs=tokens,
        check_vma=False,
    )
```

```python
import functools

import jax
import jax.numpy as jnp
from jax import lax
from jax.experimental import pallas as pl
from jax.experimental.pallas import tpu as pltpu
from jax.sharding import PartitionSpec as P

HEAD = 128
THETA = 10000
LOG2E = 1.4426950408889634
WIDE = 256
SLOTS = 6
STRIP = 512
OUT = 512
LAST = 1024
MESH = pl.DeviceIdType.MESH


def _dot(a, b, ca=1, cb=0):
    return lax.dot_general(a, b, (((ca,), (cb,)), ((), ())), preferred_element_type=jnp.float32)


def _kernel(nz, x_ref, gain_ref, wq_ref, wk_ref, wv_ref, wo_ref, y_ref, x_s, a_s, pool, wo_s, kv_s, qa_s, qb_s, top_s, mix_s, acc_s, own_s,
            oth_s, y_s, cos_s, sin_s, gain_s, w_sem, wo_sem, x_sem, ring_send, ring_recv, rest_recv, seen_send, seen_recv, y_sem):
    me = lax.axis_index("sp")
    core, z = lax.rem(me, 2), lax.div(me, 2)
    mate = me + 1 - 2 * core
    right, left = 2 * lax.rem(z + 1, nz) + core, 2 * lax.rem(z + nz - 1, nz) + core
    own, d = x_ref.shape
    both = 2 * own
    groups = kv_s.shape[1]
    per = groups // 2
    g = qa_s.shape[0] // per
    rows = own_s.shape[2]
    half = y_s.shape[1]
    far = nz // 2
    tiles = groups * g * HEAD // WIDE
    e = HEAD**-0.5 * LOG2E

    def load(ref, column, slot):
        return pltpu.make_async_copy(ref.at[:, pl.ds(pl.multiple_of(column, WIDE), WIDE)], pool.at[slot], w_sem.at[slot])

    def wq_tile(i):
        return load(wq_ref, core * (groups * g * HEAD) + i * WIDE, lax.rem(i + 2 * groups // 2, SLOTS))

    def wk_tile(p):
        return load(wk_ref, core * (groups * HEAD) + p * WIDE, 2 * p)

    def wv_tile(p):
        return load(wv_ref, core * (groups * HEAD) + p * WIDE, 2 * p + 1)

    def first_head(h, i, row=slice(None)):
        column = pl.ds(pl.multiple_of(core * (groups * HEAD) + h * HEAD, HEAD), HEAD)
        slot = i if h == 0 else groups + i
        return pltpu.make_async_copy((wk_ref, wv_ref)[i].at[row, column], pool.at[i, row, pl.ds(h * HEAD, HEAD)], w_sem.at[slot])

    def start_head(h):
        for part in range(4):
            for i in range(2):
                first_head(h, i, pl.ds(part * (d // 4), d // 4)).start()

    def wo_tile(s, o):
        who = core if o == 0 else 1 - core
        row = pl.multiple_of(who * (2 * rows) + s * rows, 128)
        return pltpu.make_async_copy(wo_ref.at[pl.ds(row, rows), pl.ds(pl.multiple_of(core * half, 128), half)], wo_s.at[s, o], wo_sem.at[s])

    def wo_both(s):
        return pltpu.make_async_copy(wo_s.at[s], wo_s.at[s], wo_sem.at[s])

    def to(src, dst, send, recv, device):
        return pltpu.make_async_remote_copy(src_ref=src, dst_ref=dst, send_sem=send, recv_sem=recv, device_id={"sp": device}, device_id_type=MESH)

    def hop(k, h, way):
        src, dst = (k - 1, k) if way == 0 else (lax.rem(nz + 1 - k, nz), nz - k)
        return to(kv_s.at[src, h], kv_s.at[dst, h], ring_send.at[way, k - 1], ring_recv.at[way, k - 1, h], right if way == 0 else left)

    def part_hop(h, way, i):
        k = far - 1
        src, dst = (k - 1, k) if way == 0 else (nz + 1 - k, nz - k)
        recv = (ring_recv if i == way else rest_recv).at[(way, k - 1, h) if i == way else (way, h)]
        return to(kv_s.at[src, h, i], kv_s.at[dst, h, i], ring_send.at[way, k - 1], recv, right if way == 0 else left)

    def last_hop(h, way):
        src = far - 1 if way == 0 else nz + 1 - far
        return to(kv_s.at[src, h, way], kv_s.at[far, h, way], ring_send.at[way, far - 1], ring_recv.at[way, far - 1, h], right if way == 0 else left)

    x_own = pltpu.make_async_copy(x_ref, x_s.at[core], x_sem.at[0])
    x_mate = to(x_ref, x_s.at[core], x_sem.at[1], x_sem.at[2], mate)

    def needs(r, k, way):
        return r >= k if way == 0 else (r + k >= nz) | (r + k < far)

    def gets(k, way):
        return needs(z, k, way)

    def gives(k, way):
        return needs(lax.rem(z + 1, nz) if way == 0 else lax.rem(z + nz - 1, nz), k, way)

    def half_hop(h, way, part):
        row = pl.ds(pl.multiple_of((core if part == 0 else 1 - core) * own, own), own)
        src, dst = kv_s.at[0, h, :, row], kv_s.at[1 if way == 0 else nz - 1, h, :, row]
        return to(src, dst, ring_send.at[way, 0], ring_recv.at[way, 0, h], right if way == 0 else left)

    def when(cond, *copies):
        @pl.when(cond)
        def _():
            for act in copies:
                act()

    gain = pltpu.make_async_copy(gain_ref, gain_s, x_sem.at[3])
    x_own.start()
    gain.start()
    start_head(0)
    barrier = pltpu.get_barrier_semaphore()
    for device in (mate, left, right):
        pl.semaphore_signal(barrier, inc=1, device_id={"sp": device}, device_id_type=MESH)

    with jax.named_scope("tables"):
        place = lax.broadcasted_iota(jnp.int32, (both, HEAD), 0) + z * both
        lane = lax.broadcasted_iota(jnp.int32, (1, HEAD), 1)
        freq = jnp.ones((1, HEAD), jnp.float32)
        for bit in range((HEAD // 2).bit_length() - 1):
            freq = jnp.where(lax.rem(lax.div(lane, 2**bit), 2) == 1, freq * THETA ** (-(2**bit) / (HEAD // 2)), freq)
        angle = place.astype(jnp.float32) * freq
        sign = jnp.where(lane < HEAD // 2, -1.0, 1.0)
        cos_s[...] = jnp.cos(angle)
        start_head(1)
        sin_s[...] = jnp.sin(angle) * sign

    def meet():
        with jax.named_scope("barrier"):
            pl.semaphore_wait(barrier, 3)
        x_mate.start()

    when(z >= far, meet)

    def norm(who):
        def chunk(r, _):
            wide = x_s[who, pl.ds(pl.multiple_of(r * 16, 16), 16), :].astype(jnp.float32)
            scale = lax.rsqrt(jnp.mean(wide * wide, -1, keepdims=True) + 1e-6)
            a = (wide * scale * gain_s[...].astype(jnp.float32).reshape(1, d)).astype(jnp.bfloat16)
            a_s[pl.ds(pl.multiple_of(who * own + r * 16, 16), 16), :] = a

        lax.fori_loop(0, own // 16, chunk, None, unroll=8)

    def turn(t, rows=slice(None)):
        t = t.astype(jnp.bfloat16).astype(jnp.float32)
        return (t * cos_s[rows] + pltpu.roll(t, HEAD // 2, 1) * sin_s[rows]).astype(jnp.bfloat16)

    def keys_values(p, here, first):
        if first:
            wk_tile(p).wait()
            wv_tile(p).wait()
        a = a_s[here]
        keys, values = _dot(a, pool[2 * p]), _dot(a, pool[2 * p + 1]).astype(jnp.bfloat16)
        for i in range(2):
            at = slice(i * HEAD, (i + 1) * HEAD)
            kv_s[0, 2 * p + i, 0, here] = turn(keys[:, at], here)
            kv_s[0, 2 * p + i, 1, here] = values[:, at]

    for part in range(2):
        who = core if part == 0 else 1 - core
        here = pl.ds(pl.multiple_of(who * own, own), own)
        with jax.named_scope("norm"):
            if part == 0:
                x_own.wait()
                gain.wait()
            else:
                x_mate.wait_recv()
            norm(who)
        if part == 0:
            wk_tile(1).start()
            wv_tile(1).start()
        with jax.named_scope("kv0"):
            if part == 0:
                for h in range(per):
                    for i in range(2):
                        first_head(h, i).wait()
                    at = slice(h * HEAD, (h + 1) * HEAD)
                    a = a_s[here]
                    keys, values = _dot(a, pool[0, :, at]), _dot(a, pool[1, :, at])
                    kv_s[0, h, 0, here] = turn(keys, here)
                    kv_s[0, h, 1, here] = values.astype(jnp.bfloat16)
                    if h == 0:
                        when(z < far, meet)
                    for way in range(2):
                        when(gives(1, way), half_hop(h, way, part).start)
            else:
                keys_values(0, here, False)
                for way in range(2):
                    when(gives(1, way), *[half_hop(h, way, part).start for h in range(per)])
        for i in range(2):
            wq_tile(2 * part + i).start()
    with jax.named_scope("kv1"):
        for part in range(2):
            who = core if part == 0 else 1 - core
            keys_values(1, pl.ds(pl.multiple_of(who * own, own), own), part == 0)
    for i in range(2):
        wq_tile(SLOTS - 2 + i).start()

    def start_own(h):
        for way in range(2):
            when(gives(1, way), hop(1, h, way).start)

    start_own(per)

    def queries(ref, i, tile):
        got = _dot(a_s[...], pool[lax.rem(tile + groups, SLOTS)])
        for n in range(2):
            ref[2 * i + n] = turn(got[:, n * HEAD : (n + 1) * HEAD])

    def forward(k, h):
        for way in range(2):
            more = gives(k + 1, way)
            when(more & (k + 1 < far - 1), hop(k + 1, h, way).start)
            when(more & (k + 1 == far - 1), part_hop(h, way, way).start, part_hop(h, way, 1 - way).start)
            when(more & (k + 1 == far), last_hop(h, way).start)

    def arrived(k, h):
        with jax.named_scope("wait"):
            for way in range(2):
                when(gets(k, way) & (k < far - 1), hop(k, h, way).wait_recv)
                when(gets(k, way) & (k == far - 1), part_hop(h, way, way).wait_recv)
        forward(k, h)

    def first_queries(i, _):
        for n in range(2):
            wq_tile(2 * i + n).wait()
        for n in range(2):
            queries(qa_s, 2 * i + n, 2 * i + n)
        for n in range(2):
            wq_tile(2 * i + n + SLOTS).start()
        for j in range(per):
            when(i == 1 + j, lambda: arrived(1, j))

    with jax.named_scope("qa"):
        lax.fori_loop(0, tiles // 4, first_queries, None)
    for s in range(2):
        for o in range(2):
            wo_tile(s, o).start()

    def attend(q_s, j, h, slots, diagonal=False, beside=None):
        keys = [kv_s[n, h, 0] for n in slots]
        values = jnp.concatenate([kv_s[n, h, 1].T for n in slots], axis=1)
        values = jnp.concatenate([values, jnp.ones((8, values.shape[1]), values.dtype)], axis=0)
        n = STRIP // both
        strips = range(0, g * both, STRIP)
        scores = []
        for at in strips:
            q = q_s[pl.ds(g * j + at // both, n)].reshape(STRIP, HEAD)
            scores.append([_dot(k, q, 1, 1) for k in keys])
        if beside is not None:
            beside()
        weights, keeps = [], []
        for at, parts in zip(strips, scores):
            if diagonal:
                seen = lax.rem(lax.broadcasted_iota(jnp.int32, (both, STRIP), 1), both) >= lax.broadcasted_iota(jnp.int32, (both, STRIP), 0)
                parts = [jnp.where(seen, parts[0], -jnp.inf)]
            old = None if diagonal else top_s[j, :, at : at + STRIP]
            top = functools.reduce(jnp.maximum, [s.max(axis=0, keepdims=True) for s in parts] + ([] if diagonal else [old]))
            top_s[j, :, at : at + STRIP] = top
            weights.append(jnp.concatenate([jnp.exp2((s - top) * e).astype(jnp.bfloat16) for s in parts], axis=0))
            keeps.append(None if diagonal else jnp.exp2((old - top) * e))
        for at, w, keep in zip(strips, weights, keeps):
            got = _dot(values, w)
            mix_s[j, :, at : at + STRIP] = got if diagonal else mix_s[j, :, at : at + STRIP] * keep + got

    def span(h):
        return slice((h % per) * g * HEAD, (h % per + 1) * g * HEAD)

    def seen(h):
        part = (h // per, slice(None), pl.ds((h % per) * g * HEAD, g * HEAD))
        return to(own_s.at[part], oth_s.at[part], seen_send.at[0], seen_recv.at[max(h - per + 1, 0)], mate)

    def seen_all(s):
        return to(own_s.at[s], oth_s.at[s], seen_send.at[0], seen_recv.at[0], mate)

    def finish(h):
        j = h % per
        with jax.named_scope("finish"):
            for n in range(g):
                at = slice(n * both, (n + 1) * both)
                out = mix_s[j, :HEAD, at] * (1 / mix_s[j, HEAD : HEAD + 1, at])
                column = (j * g + n) * HEAD
                own_s[h // per, :, column : column + HEAD] = out.T.astype(jnp.bfloat16)
        seen(h).start()

    def stage(s, begin, steps, ready, beside):
        base = s * per
        q_s = (qa_s, qb_s)[s]

        def arrive(n, _):
            k, j = 1 + lax.div(n, per), lax.rem(n, per)
            h = base + j
            if s > 0:
                when(n == 1, *[lambda: arrived(1, base + i) for i in range(1, per)])
            when(n >= per, lambda: arrived(k, h))
            if s == 0:
                @pl.when(n == (far - 1) * per - 1)
                def _():
                    for later in range(per + 1, groups):
                        start_own(later)
                    arrived(1, per)

            with jax.named_scope("diag"):
                @pl.when(k == 1)
                def _():
                    attend(q_s, j, h, [0], diagonal=True)

            ready(n - begin)
            with jax.named_scope("rest"):
                for way in range(2):
                    when(gets(k, way) & (k == far - 1), part_hop(h, way, 1 - way).wait_recv)

            def work(busy):
                todo = (lambda: beside(n - begin)) if busy else None
                with jax.named_scope("att"):
                    @pl.when(z + k >= nz)
                    def _():
                        attend(q_s, j, h, [k, nz - k], beside=todo)

                    @pl.when((z + k < nz) & (z >= k))
                    def _():
                        attend(q_s, j, h, [k], beside=todo)

                    if busy:
                        when(z < k, todo)

            if steps == (far - 1) * per:
                work(True)
            else:
                busy = (n >= begin) & (n < begin + steps)
                when(busy, lambda: work(True))
                when(jnp.logical_not(busy), lambda: work(False))

        lax.fori_loop(0, (far - 1) * per, arrive, None)

    def end(h):
        q_s = (qa_s, qb_s)[h // per]
        with jax.named_scope("end"):
            @pl.when(z >= far)
            def _():
                for way in range(2):
                    last_hop(h, way).wait_recv()
                attend(q_s, h % per, h, [far])
        finish(h)

    def column_tile(ct):
        return pl.ds(pl.multiple_of(ct * OUT, OUT), OUT)

    def project(h, o, at):
        i = span(h)
        return _dot((own_s, oth_s)[o][h // per, :, i], wo_s[h // per, o, i, at])

    stage(0, 0, tiles // 2, lambda n: wq_tile(tiles // 2 + n).wait(), lambda n: queries(qb_s, n, tiles // 2 + n))
    for h in range(per):
        end(h)

    wo_both(0).wait()

    def first_half(n):
        at = column_tile(n)
        acc_s[:, at] = _dot(own_s[0], wo_s[0, 0, :, at]) + _dot(oth_s[0], wo_s[0, 1, :, at])
        for i in range(2):
            x = x_s[i, :, pl.ds(pl.multiple_of(core * half + n * OUT, OUT), OUT)].astype(jnp.float32)
            acc_s[i * own : (i + 1) * own, at] += x

    stage(1, 1, half // OUT, lambda n: when(n == 0, seen_all(0).wait_recv), first_half)

    wo_both(1).wait()

    def passed(work, width=OUT):
        for ct in range(half // width):
            work(ct, slice(ct * width, (ct + 1) * width))

    def own_first(ct, at):
        acc_s[:, at] += project(per, 0, at)

    def own_second(ct, at):
        acc_s[:, at] += project(per + 1, 0, at) + project(per, 1, at)

    def columns(width, at=0):
        return pl.ds(pl.multiple_of(core * half + at, OUT), width)

    def y_mate(width, at=0):
        return to(y_s.at[:, pl.ds(at, width)], y_ref.at[:, columns(width, at)], y_sem.at[0], y_sem.at[1], mate)

    def last(who, at):
        here = pl.ds(pl.multiple_of(who * own, own), own)
        i = span(per + 1)
        return (acc_s[here, at] + _dot(oth_s[1, here, i], wo_s[1, 1, i, at])).astype(jnp.bfloat16)

    def mate_rows(ct, at):
        y_s[:, at] = last(1 - core, at)
        y_mate(LAST, ct * LAST).start()

    def own_rows(ct, at):
        y_ref[:, columns(LAST, ct * LAST)] = last(core, at)

    end(per)
    with jax.named_scope("tail0"):
        passed(own_first)
    end(per + 1)
    seen(per).wait_recv()
    with jax.named_scope("tail1"):
        passed(own_second)
    seen(per + 1).wait_recv()
    with jax.named_scope("tail2"):
        passed(mate_rows, LAST)
        passed(own_rows, LAST)
    with jax.named_scope("sent"):
        x_mate.wait_send()
        to(own_s, oth_s, seen_send.at[0], seen_recv.at[0], mate).wait_send()
        for way in range(2):
            for k in range(1, far):
                when(gives(k, way), to(kv_s.at[0], kv_s.at[1], ring_send.at[way, k - 1], ring_recv.at[way, k - 1, 0], mate).wait_send)
            last = to(kv_s.at[0, :, way], kv_s.at[1, :, way], ring_send.at[way, far - 1], ring_recv.at[way, far - 1, 0], mate)
            when(gives(far, way), last.wait_send)
    with jax.named_scope("ywait"):
        y_mate(half).wait()


def solution(mesh):
    nz = mesh.shape["sp"] // 2

    def step(x, gain, wq, wk, wv, wo):
        own, d = x.shape
        both = 2 * own
        heads, groups = wq.shape[1] // HEAD // 2, wk.shape[1] // HEAD // 2
        g, per, half = heads // groups, groups // 2, d // 2
        rows = heads * HEAD // 2
        far = nz // 2
        hbm = pl.BlockSpec(memory_space=pl.ANY)
        low = jnp.bfloat16
        dma = pltpu.SemaphoreType.DMA
        return pl.pallas_call(
            functools.partial(_kernel, nz),
            out_shape=pltpu.VMEM((own, d), low),
            in_specs=[hbm] * 6,
            out_specs=pl.BlockSpec(memory_space=pltpu.VMEM),
            scratch_shapes=[
                pltpu.VMEM((2, own, d), low),
                pltpu.VMEM((both, d), low),
                pltpu.VMEM((SLOTS, d, WIDE), low),
                pltpu.VMEM((2, 2, rows, half), low),
                pltpu.VMEM((nz, groups, 2, both, HEAD), low),
                pltpu.VMEM((heads // 2, both, HEAD), low),
                pltpu.VMEM((heads // 2, both, HEAD), low),
                pltpu.VMEM((per, 1, g * both), jnp.float32),
                pltpu.VMEM((per, HEAD + 8, g * both), jnp.float32),
                pltpu.VMEM((both, half), jnp.float32),
                pltpu.VMEM((2, both, rows), low),
                pltpu.VMEM((2, both, rows), low),
                pltpu.VMEM((own, half), low),
                pltpu.VMEM((both, HEAD), jnp.float32),
                pltpu.VMEM((both, HEAD), jnp.float32),
                pltpu.VMEM((d,), low),
                dma((SLOTS,)),
                dma((2,)),
                dma((4,)),
                dma((2, far)),
                dma((2, far, groups)),
                dma((2, groups)),
                dma((1,)),
                dma((1 + groups - per,)),
                dma((2,)),
            ],
            compiler_params=pltpu.CompilerParams(collective_id=0, has_side_effects=True, vmem_limit_bytes=62 * 2**20),
        )(x, gain, wq, wk, wv, wo)

    tokens, whole = P(("dp", "sp"), None), P(None, None)
    return jax.shard_map(
        step,
        mesh=mesh,
        in_specs=(tokens, P(None), whole, whole, whole, whole),
        out_specs=tokens,
        check_vma=False,
    )
```
